32 devices in a mesh: head: 4 (over y, core), seq: 8 (over z, x).
Axes of the slice: x: 2, y: 2, z: 4, core: 2. Of those that a mesh axis runs over, the one named last changes fastest.
Arguments:
- queries: bfloat16 [2, 4, 32, 128], P(None, None, ('head', 'seq')), may hold values from -16 to 16
- keys: bfloat16 [2, 4, 16384, 128], P(None, 'head', 'seq'), may hold values from -6 to 6
- values: bfloat16 [2, 4, 16384, 128], P(None, 'head', 'seq'), may hold values from -6 to 6
- indices: int32 [4, 8, 1024], P('head'), may hold values from 0 to 16383, as said below
- sizes: int32 [4, 8], P('head'), may hold values from 128 to 1024, as said below
- owners: int32 [4, 8], P('head'), may hold values from 0 to 7, as said below
Outputs:
- compact_values: bfloat16 [4, 24, 1024, 128], P('head', 'seq')
The draws below stay inside these ranges and needn't reach their ends.
Inputs may be any that keep to these rules, and one draw needn't show every extreme that they name: `indices`: in each row of a head and fit, the 1024 positions are distinct and the first two are 0 and 1; only the first sizes[h,f] are used. `sizes`: multiples of 128; in each head one fit has 1024. `owners`: no index owns more than 3 fits of a head; in each head one index owns exactly 3.
All inputs are finite; a program needn't handle non-finite values.
Results may differ from the reference program's by a relative error of at most 0.008.
Values may be sent and summed in bfloat16 or wider, within the bound.
A program may use at most 128 MiB of HBM per device.

```python
import jax
import jax.numpy as jnp
from jax import lax

HD = 128
LAYERS = 2
FITS_LAYER = 4
CMAX = 1024
SLOTS = 3
KVH = 4
SEQ_LEN = 16384
QUERIES = 32
FITS = 8
STEP = 128
N_SEQ = 8


def draw_keys(key, part):
    base = jax.random.normal(jax.random.fold_in(key, 1), (LAYERS, KVH, SEQ_LEN, HD), jnp.float32)
    return jnp.clip(base, -6.0, 6.0).astype(jnp.bfloat16)


def draw_queries(key, part):
    base = 2.5 * jax.random.normal(jax.random.fold_in(key, 3), (LAYERS, KVH, QUERIES, HD), jnp.float32)
    return jnp.clip(base, -16.0, 16.0).astype(jnp.bfloat16)


def draw_indices(key, part):
    streams = jax.random.split(jax.random.fold_in(key, 6), KVH * FITS)
    picked = jax.vmap(lambda one: jax.random.permutation(one, SEQ_LEN - 2)[:CMAX - 2] + 2)(streams)
    lead = jnp.broadcast_to(jnp.array([0, 1], jnp.int32), (KVH * FITS, 2))
    return jnp.concatenate([lead, picked.astype(jnp.int32)], axis=1).reshape(KVH, FITS, CMAX)


def draw_sizes(key, part):
    units = jax.random.randint(jax.random.fold_in(key, 7), (KVH, FITS), 1, 9)
    chosen = jax.random.randint(jax.random.fold_in(key, 8), (KVH, 1), 0, FITS)
    units = jnp.where(jnp.arange(FITS)[None, :] == chosen, 8, units)
    return (units * STEP).astype(jnp.int32)


def owner_row(one):
    busy = jax.random.randint(jax.random.fold_in(one, 1), (), 0, N_SEQ)
    rest = jax.random.permutation(jax.random.fold_in(one, 2), N_SEQ - 1)
    rest = jnp.where(rest >= busy, rest + 1, rest)[:FITS - SLOTS]
    listed = jnp.concatenate([jnp.full((SLOTS,), busy), rest])
    order = jax.random.permutation(jax.random.fold_in(one, 3), FITS)
    return listed[order].astype(jnp.int32)


def draw_owners(key, part):
    streams = jax.random.split(jax.random.fold_in(key, 9), KVH)
    return jax.vmap(owner_row)(streams)


def levels(own_key, extent, shards, low, top_value):
    level, own = 1.0, jax.random.fold_in(own_key, 6)
    for position, shards_of in shards:
        draws = jnp.exp(jax.random.uniform(jax.random.fold_in(own, position), (shards_of,), jnp.float32, low / len(shards), top_value / len(shards)))
        level = level * jnp.repeat(draws, extent[position] // shards_of).reshape([-1 if axis == position else 1 for axis in range(len(extent))])
    return level


def noise(own_key, shape, scale, limit, cuts=(), kind=jnp.bfloat16):
    entries = scale * jax.random.normal(own_key, shape, jnp.float32)
    if cuts:
        entries = entries * levels(own_key, shape, cuts, -0.22, 0.18)
    return jnp.clip(entries, -limit, limit).astype(kind)


def setup_inputs(seed: int = 0) -> dict:
    splits = jax.random.split(jax.random.key(seed), 7)
    queries = draw_queries(jax.random.fold_in(splits[6], 71), 0)
    keys = draw_keys(jax.random.fold_in(splits[6], 71), 0)
    values = noise(splits[2], (LAYERS, KVH, SEQ_LEN, HD), 1.0, 6.0, ((1, 4), (2, 8)))
    indices = draw_indices(jax.random.fold_in(splits[6], 71), 0)
    sizes = draw_sizes(jax.random.fold_in(splits[6], 71), 0)
    owners = draw_owners(jax.random.fold_in(splits[6], 71), 0)
    return {"queries": queries, "keys": keys, "values": values, "indices": indices, "sizes": sizes, "owners": owners}


RIDGE = 0.3

def solve_fit(query_rows, target_rows, compact, size):
    scale = query_rows.shape[-1] ** (-0.5)
    width = compact.shape[0]
    scores = lax.dot_general(query_rows.astype(jnp.float32), compact.astype(jnp.float32), (((1,), (1,)), ((), ())), preferred_element_type=jnp.float32) * scale
    live = jnp.arange(width, dtype=jnp.int32) < size
    scores = jnp.where(live[None, :], scores, -jnp.inf)
    peak = jnp.max(scores, axis=1)
    expo = jnp.exp(scores - peak[:, None])
    probs = (expo / jnp.sum(expo, axis=1)[:, None]).astype(jnp.bfloat16)
    gram = lax.dot_general(probs.astype(jnp.float32), probs.astype(jnp.float32), (((0,), (0,)), ((), ())), preferred_element_type=jnp.float32)
    rhs = lax.dot_general(probs.astype(jnp.float32), target_rows.astype(jnp.float32), (((0,), (0,)), ((), ())), preferred_element_type=jnp.float32)
    ridge = RIDGE * jnp.trace(gram) / size.astype(jnp.float32)
    system = gram + jnp.diag(jnp.where(live, ridge, jnp.float32(1.0)))
    factor = jnp.linalg.cholesky(system)
    solution = jax.scipy.linalg.cho_solve((factor, True), rhs)
    return solution.astype(jnp.bfloat16)

def attend(query_rows, key_rows, value_rows):
    scale = query_rows.shape[-1] ** (-0.5)
    scores = jnp.dot(query_rows.astype(jnp.float32), key_rows.astype(jnp.float32).T.astype(jnp.float32), preferred_element_type=jnp.float32) * scale
    peak = jnp.max(scores, axis=1)
    weights = jnp.exp(scores - peak[:, None])
    total = jnp.sum(weights, axis=1)
    rounded = lax.optimization_barrier(weights.astype(jnp.bfloat16))
    numer = jnp.dot(rounded.astype(jnp.float32), value_rows.astype(jnp.float32), preferred_element_type=jnp.float32)
    return (numer / total[:, None]).astype(jnp.bfloat16)

def reference(queries, keys, values, indices, sizes, owners):
    layers, heads = (keys.shape[0], keys.shape[1])
    width = keys.shape[3]
    flat_q = queries.reshape(layers * heads, QUERIES, width)
    flat_k = keys.reshape(layers * heads, SEQ_LEN, width)
    flat_v = values.reshape(layers * heads, SEQ_LEN, width)
    targets = lax.map(lambda group: attend(group[0], group[1], group[2]), (flat_q, flat_k, flat_v))
    targets = targets.reshape(layers, heads, QUERIES, width)
    head_ids = jnp.repeat(jnp.arange(heads, dtype=jnp.int32), FITS)
    fit_list = jnp.tile(jnp.arange(FITS, dtype=jnp.int32), heads)

    def one_fit(pair):
        head, fit = pair
        layer = fit // FITS_LAYER
        compact = jnp.take(keys[layer, head], indices[head, fit], axis=0)
        return solve_fit(queries[layer, head], targets[layer, head], compact, sizes[head, fit])
    solutions = lax.map(one_fit, (head_ids, fit_list)).reshape(heads, FITS, CMAX, width)
    fit_ids = jnp.arange(FITS, dtype=jnp.int32)
    same = owners[:, :, None] == owners[:, None, :]
    before = fit_ids[:, None] > fit_ids[None, :]
    earlier = jnp.sum((same & before[None]).astype(jnp.int32), axis=2)
    slot = (owners * SLOTS + earlier).astype(jnp.int32)
    result = jnp.zeros((heads, N_SEQ * SLOTS, CMAX, width), jnp.bfloat16)
    return result.at[jnp.arange(heads, dtype=jnp.int32)[:, None], slot].set(solutions)
```

```python
import jax
import jax.numpy as jnp
from jax import lax
from jax.experimental import pallas as pl
from jax.experimental.pallas import tpu as pltpu
from jax.sharding import PartitionSpec as P

FITS_LAYER = 4
SLOTS = 3
RIDGE = 0.3
LANES = 128
FAR = -(2.0**100)
LOG2E = 1.4426950408889634
PAIR = 2
BAND = 32

SUBLANES = 8
MESH = pl.DeviceIdType.MESH
NT = (((1,), (1,)), ((), ()))
TN = (((0,), (0,)), ((), ()))


def solve_rows(system, target):
    rows = system.shape[0]
    row = lax.broadcasted_iota(jnp.int32, (rows, 1), 0)
    if rows <= 64:
        for k in range(rows):
            inverse = 1.0 / system[k : k + 1, k : k + 1]
            pivot_s = system[k : k + 1, :] * inverse
            pivot_t = target[k : k + 1, :] * inverse
            column = jnp.where(row == k, system[:, k : k + 1] - 1.0, system[:, k : k + 1])
            system = system - column * pivot_s
            target = target - column * pivot_t
        return target
    lane = lax.broadcasted_iota(jnp.int32, (1, rows), 1)

    def step(k, state):
        system, target = state
        column = jnp.sum(jnp.where(lane == k, system, 0.0), axis=1, keepdims=True)
        here = row == k
        inverse = 1.0 / jnp.sum(jnp.where(here, column, 0.0), axis=0, keepdims=True)
        pivot_s = jnp.sum(jnp.where(here, system, 0.0), axis=0, keepdims=True) * inverse
        pivot_t = jnp.sum(jnp.where(here, target, 0.0), axis=0, keepdims=True) * inverse
        column = jnp.where(here, column - 1.0, column)
        return system - column * pivot_s, target - column * pivot_t

    return lax.fori_loop(0, rows, step, (system, target))[1]


def split_exponent(block, capacity):
    tail = block[:, capacity:].astype(jnp.float32)
    return block[:, :capacity].astype(jnp.float32), tail[:, 0:1] + tail[:, 64:65]


def joined_exponent(expo, top, lane):
    high = top.astype(jnp.bfloat16)
    low = (top - high.astype(jnp.float32)).astype(jnp.bfloat16)
    tail = jnp.where(lane < 64, high.astype(jnp.float32), low.astype(jnp.float32))
    return jnp.concatenate([expo.astype(jnp.bfloat16), tail.astype(jnp.bfloat16)], axis=1)


def enter(axes):
    barrier = pltpu.get_barrier_semaphore()
    total = 0
    for axis in axes:
        me, size = lax.axis_index(axis), lax.axis_size(axis)
        for step in range(1, size):
            pl.semaphore_signal(
                barrier, inc=1, device_id={axis: lax.rem(me + step, size)}, device_id_type=MESH
            )
        total += size - 1
    pl.semaphore_wait(barrier, total)


def send(source, target, send_sem, recv_sem, axis, peer):
    return pltpu.make_async_remote_copy(
        src_ref=source,
        dst_ref=target,
        send_sem=send_sem,
        recv_sem=recv_sem,
        device_id={axis: peer},
        device_id_type=MESH,
    )


def fit_kernel(
    sizes_ref, q_in, k_hbm, v_hbm, idx_ref, p_ref, x_ref,
    piece, column, table, k_ref, v_ref, s_ref, g_ref, high_ref, low_ref, t_ref, part, part_in, chunk_mine, chunks, e_out, e_in, z_out, z_in,
    p_mine, p_all, x_mine, x_all,
    load, send_head, recv_head, send_seq, recv_seq, send_part, recv_part, send_chunk, recv_chunk, send_e, recv_e, send_z, recv_z,
    send_p, recv_p, send_f, recv_f, send_x, recv_x,
):
    layers, local_len, width = k_ref.shape
    fits, capacity = idx_ref.shape
    heads, my_head = lax.axis_size("head"), lax.axis_index("head")
    groups, me = lax.axis_size("seq"), lax.axis_index("seq")
    rows = groups * heads
    outer, inner = me // PAIR, lax.rem(me, PAIR)
    outers, half = groups // PAIR, fits // PAIR
    partner = outer * PAIR + 1 - inner
    fit_mine = jnp.minimum(me, fits - 1)
    chunk = layers * rows // groups
    start = me * local_len
    lane = lax.broadcasted_iota(jnp.int32, (rows, LANES), 1)
    exact = outers == half

    loads = [
        pltpu.make_async_copy(k_hbm, k_ref, load.at[0]),
        pltpu.make_async_copy(v_hbm, v_ref, load.at[1]),
    ]
    for copy in loads:
        copy.start()
    drawn_rows = q_in[...].astype(jnp.float32)
    for head in range(heads):
        for layer in range(layers):
            at = layer * heads + head
            piece[head, layer : layer + 1, :] = drawn_rows[at : at + 1]
        piece[head, layers:, :] = jnp.zeros((SUBLANES - layers, width), jnp.float32)
    enter(("head", "seq"))
    near = heads * SUBLANES
    column[pl.ds(pl.multiple_of(my_head * SUBLANES, SUBLANES), SUBLANES), :] = piece[my_head]
    first, second = [], []
    for step in range(1, heads):
        peer = lax.rem(my_head + step, heads)
        first.append(
            send(
                piece.at[peer],
                column.at[pl.ds(pl.multiple_of(my_head * SUBLANES, SUBLANES), SUBLANES), :],
                send_head.at[step], recv_head.at[step], "head", peer,
            )
        )
        first[-1].start()
    for copy in first:
        copy.wait_recv()
    for step in range(1, groups):
        peer = lax.rem(me + step, groups)
        second.append(
            send(
                column, table.at[pl.ds(pl.multiple_of(me * near, near), near), :],
                send_seq.at[step], recv_seq.at[step], "seq", peer,
            )
        )
        second[-1].start()
    table[pl.ds(pl.multiple_of(me * near, near), near), :] = column[...]
    for copy in second:
        copy.wait_recv()
    for copy in loads:
        copy.wait()

    for layer in range(layers):
        query_rows = table[pl.ds(layer, rows, stride=SUBLANES), :].astype(jnp.bfloat16)
        scores = lax.dot_general(
            query_rows, k_ref[layer], NT, preferred_element_type=jnp.float32
        ) * (width ** (-0.5) * LOG2E)
        s_ref[layer] = scores
        peak = jnp.max(scores, axis=1, keepdims=True)
        weights = jnp.exp2(scores - peak)
        total = jnp.sum(weights, axis=1, keepdims=True)
        numer = jnp.dot(
            weights.astype(jnp.bfloat16), v_ref[layer], preferred_element_type=jnp.float32
        )
        side = jnp.where(lane < 64, total, peak)
        for at in range(rows // chunk):
            slot = layer * (rows // chunk) + at
            part[slot, 0] = numer[at * chunk : (at + 1) * chunk]
            part[slot, 1] = side[at * chunk : (at + 1) * chunk]

    def produce(fit):
        layer = fit // FITS_LAYER
        size = sizes_ref[0, fit]
        offset = idx_ref[pl.ds(fit, 1), :] - start
        position = lax.broadcasted_iota(jnp.int32, (1, capacity), 1)
        inside = (offset >= 0) & (offset < local_len) & (position < size)
        high_ref[...] = jnp.broadcast_to(
            jnp.where(inside, offset >> 7, -1), (SUBLANES, capacity)
        )
        low_ref[...] = jnp.broadcast_to(offset & (LANES - 1), (SUBLANES, capacity))
        band = min(rows, BAND)

        def one_band(base_row):
            def one_tile(tile, top):
                base = pl.multiple_of(tile * LANES, LANES)
                high = high_ref[:, pl.ds(base, LANES)]
                low = low_ref[:, pl.ds(base, LANES)]
                picked = [jnp.full((SUBLANES, LANES), FAR, jnp.float32)] * (band // SUBLANES)
                for block in range(local_len // LANES):
                    here = high == block
                    for group in range(band // SUBLANES):
                        scored = s_ref[
                            layer,
                            pl.ds(base_row + group * SUBLANES, SUBLANES),
                            block * LANES : (block + 1) * LANES,
                        ]
                        found = jnp.take_along_axis(
                            scored, low, axis=1, mode="promise_in_bounds"
                        )
                        picked[group] = jnp.where(here, found, picked[group])
                joined = jnp.concatenate(picked, axis=0)
                g_ref[pl.ds(base_row, band), pl.ds(base, LANES)] = joined
                return jnp.maximum(top, joined)

            top = lax.fori_loop(
                0,
                capacity // LANES,
                one_tile,
                jnp.full((band, LANES), FAR, jnp.float32),
                unroll=True if rows == band else 1,
            )
            t_ref[pl.ds(base_row, band), :] = top

        if rows == band:
            one_band(0)
        else:

            def step(at, carry):
                one_band(pl.multiple_of(at * band, band))
                return carry

            lax.fori_loop(0, rows // band, step, 0)
        top = jnp.ceil(jnp.max(t_ref[...], axis=1, keepdims=True))
        picked = g_ref[...]
        return jnp.where(picked > 0.5 * FAR, jnp.exp2(picked - top), 0.0), top

    parts = []
    for step in range(1, groups):
        peer = lax.rem(me + step, groups)
        parts.append(
            send(
                part.at[peer], part_in.at[step],
                send_part.at[step], recv_part.at[step], "seq", peer,
            )
        )
        parts[-1].start()
    part_in[0] = part[me]

    def column_of(j):
        return lax.rem(outer + 1 + j, outers) if exact else jnp.int32(j)

    across = []
    for j in range(half):
        expo, top = produce(column_of(j) * PAIR + 1 - inner)
        e_out[j] = joined_exponent(expo, top, lane)
        across.append(
            send(e_out.at[j], e_in.at[j], send_e.at[j], recv_e.at[j], "seq", partner)
        )
        if j > 0:
            across[j - 1].start()

    for copy in parts:
        copy.wait_recv()
    peak = part_in[0, 1][:, 64:65]
    for step in range(1, groups):
        peak = jnp.maximum(peak, part_in[step, 1][:, 64:65])
    numer, total = 0.0, 0.0
    for step in range(groups):
        factor = jnp.exp2(part_in[step, 1][:, 64:65] - peak)
        numer = numer + part_in[step, 0] * factor
        total = total + part_in[step, 1][:, 0:1] * factor
    merged = numer / total
    chunk_mine[...] = merged
    chunks[me] = merged
    across[half - 1].start()

    down, spread = [], []
    for j in range(half):
        dest = column_of(j)
        expo, top = produce(dest * PAIR + inner)
        if j == 0:
            for step in range(1, groups):
                peer = lax.rem(me + step, groups)
                spread.append(
                    send(
                        chunk_mine, chunks.at[me],
                        send_chunk.at[step], recv_chunk.at[step], "seq", peer,
                    )
                )
                spread[-1].start()
        across[j].wait_recv()
        other, other_top = split_exponent(e_in[j], capacity)
        both = jnp.maximum(top, other_top)
        expo = expo * jnp.exp2(top - both) + other * jnp.exp2(other_top - both)
        block = joined_exponent(expo, both, lane)
        copy = send(
            z_out.at[j], z_in.at[outer], send_z.at[j], recv_z.at[outer],
            "seq", dest * PAIR + inner,
        )
        down.append((dest, copy))
        if exact:
            if j == half - 1:
                z_in[outer] = block
            else:
                z_out[j] = block
                copy.start()
        else:
            z_out[j] = block
            pl.when(dest != outer)(copy.start)

            @pl.when(dest == outer)
            def _():
                z_in[outer] = block

    def only(condition, act):
        if exact:
            act()
        else:
            pl.when(condition)(act)

    def source_z(step):
        source = lax.rem(outer + step, outers)
        return source, send(
            z_out.at[0], z_in.at[source], send_z.at[0], recv_z.at[source], "seq", partner
        )

    def gave_p(step, target):
        return send(
            p_mine, p_all.at[fit_mine], send_p.at[step], recv_p.at[outer],
            "seq", target * PAIR + inner,
        )

    def came_p(source):
        fit = jnp.minimum(source, half - 1) * PAIR + inner
        arrival = send(
            p_mine, p_all.at[fit], send_p.at[0], recv_p.at[source], "seq", partner
        )
        onward = send(
            p_all.at[fit], p_all.at[fit], send_f.at[source], recv_f.at[source], "seq", partner
        )
        return arrival, onward

    def back_p(source):
        fit = jnp.minimum(source, half - 1) * PAIR + 1 - inner
        return send(
            p_mine, p_all.at[fit], send_f.at[source], recv_f.at[source], "seq", partner
        )

    gifts = [gave_p(step, lax.rem(outer + step, outers)) for step in range(1, outers)]
    own_onward = send(
        p_mine, p_all.at[fit_mine], send_f.at[outer], recv_f.at[outer], "seq", partner
    )
    results = [
        send(
            x_mine, x_all.at[fit_mine], send_x.at[step], recv_x.at[step],
            "seq", lax.rem(me + step, groups),
        )
        for step in range(1, groups)
    ]

    def relay():
        for step in range(1, outers):
            source = lax.rem(outer + outers - step, outers)
            arrival, onward = came_p(source)

            def pass_on():
                arrival.wait_recv()
                onward.start()

            only(source < half, pass_on)

    for copy in spread:
        copy.wait_recv()

    def work():
        for step in range(1, outers):
            source_z(step)[1].wait_recv()
        blocks = [split_exponent(z_in[source], capacity) for source in range(outers)]
        top = blocks[0][1]
        for _, other in blocks[1:]:
            top = jnp.maximum(top, other)
        probs = 0.0
        for expo, other in blocks:
            probs = probs + expo * jnp.exp2(other - top)
        probs = (probs / jnp.sum(probs, axis=1, keepdims=True)).astype(jnp.bfloat16)
        p_mine[...] = probs
        p_all[fit_mine] = probs
        gram = lax.dot_general(probs, probs, NT, preferred_element_type=jnp.float32)
        for copy in gifts:
            copy.start()
        own_onward.start()
        diagonal = lax.broadcasted_iota(jnp.int32, (rows, rows), 0) == lax.broadcasted_iota(
            jnp.int32, (rows, rows), 1
        )
        trace = jnp.sum(jnp.where(diagonal, gram, 0.0))
        ridge = RIDGE * trace / sizes_ref[0, fit_mine].astype(jnp.float32)
        span = rows // chunk
        base = (fit_mine // FITS_LAYER) * span
        target = jnp.concatenate([chunks[base + at] for at in range(span)], axis=0)
        target = target.astype(jnp.bfloat16).astype(jnp.float32)
        solved = solve_rows(jnp.where(diagonal, gram + ridge, gram), target)
        x_mine[...] = solved
        x_all[fit_mine] = solved
        for copy in results:
            copy.start()

    only(outer < half, work)
    relay()
    for copy in first + second + parts + spread + across:
        copy.wait_send()
    for j in range(half):
        dest, copy = down[j]
        if exact:
            if j < half - 1:
                copy.wait_send()
        else:
            pl.when(dest != outer)(copy.wait_send)
    for step in range(1, outers):
        source = lax.rem(outer + outers - step, outers)
        only(outer < half, gifts[step - 1].wait_send)
        only(source < half, came_p(source)[1].wait_send)
    only(outer < half, own_onward.wait_send)
    for source in range(half):
        back_p(source).wait_recv()
    for step in range(1, groups):
        source = lax.rem(me + groups - step, groups)
        only(source < fits, results[step - 1].wait_recv)
        only(outer < half, results[step - 1].wait_send)
    p_ref[...] = p_all[...]
    x_ref[...] = x_all[...]


def place_kernel(owners_ref, p_ref, x_ref, out_ref):
    me = lax.axis_index("seq")
    fits = p_ref.shape[0]
    count = jnp.int32(0)
    chosen = [jnp.int32(0)] * SLOTS
    for fit in range(fits):
        mine = owners_ref[0, fit] == me
        for slot in range(SLOTS):
            chosen[slot] = jnp.where(mine & (count == slot), fit, chosen[slot])
        count = count + mine.astype(jnp.int32)
    for slot in range(SLOTS):

        @pl.when(count > slot)
        def _():
            probs = p_ref[chosen[slot]]
            rows = x_ref[chosen[slot]]
            high = rows.astype(jnp.bfloat16)
            low = (rows - high.astype(jnp.float32)).astype(jnp.bfloat16)
            out_ref[0, slot] = lax.dot_general(
                jnp.concatenate([probs, probs], axis=0),
                jnp.concatenate([high, low], axis=0),
                TN,
                preferred_element_type=jnp.float32,
            ).astype(jnp.bfloat16)

        @pl.when(count <= slot)
        def _():
            out_ref[0, slot] = jnp.zeros(out_ref.shape[2:], jnp.bfloat16)


VMEM = pl.BlockSpec(memory_space=pltpu.VMEM)
ANY = pl.BlockSpec(memory_space=pl.ANY)
SMEM = pl.BlockSpec(memory_space=pltpu.SMEM)
PARAMS = dict(vmem_limit_bytes=60 * 1024 * 1024)


def on_device(queries, keys, values, indices, sizes, owners):
    layers, heads, count, width = queries.shape
    groups = lax.axis_size("seq")
    rows = groups * heads * count
    local_len = keys.shape[2]
    fits, capacity = indices.shape[1:]
    dma = pltpu.SemaphoreType.DMA
    outers, half = groups // PAIR, fits // PAIR
    chunk = layers * rows // groups
    packed = (rows, capacity + LANES)
    probs, solved = pl.pallas_call(
        fit_kernel,
        out_shape=(
            jax.ShapeDtypeStruct((fits, rows, capacity), jnp.bfloat16),
            jax.ShapeDtypeStruct((fits, rows, width), jnp.float32),
        ),
        in_specs=[SMEM, VMEM, ANY, ANY, VMEM],
        out_specs=(VMEM, VMEM),
        scratch_shapes=[
            pltpu.VMEM((heads, SUBLANES, width), jnp.float32),
            pltpu.VMEM((heads * SUBLANES, width), jnp.float32),
            pltpu.VMEM((rows * SUBLANES, width), jnp.float32),
            pltpu.VMEM((layers, local_len, width), jnp.bfloat16),
            pltpu.VMEM((layers, local_len, width), jnp.bfloat16),
            pltpu.VMEM((layers, rows, local_len), jnp.float32),
            pltpu.VMEM((rows, capacity), jnp.float32),
            pltpu.VMEM((SUBLANES, capacity), jnp.int32),
            pltpu.VMEM((SUBLANES, capacity), jnp.int32),
            pltpu.VMEM((rows, LANES), jnp.float32),
            pltpu.VMEM((groups, 2, chunk, width), jnp.float32),
            pltpu.VMEM((groups, 2, chunk, width), jnp.float32),
            pltpu.VMEM((chunk, width), jnp.float32),
            pltpu.VMEM((groups, chunk, width), jnp.float32),
            pltpu.VMEM((half,) + packed, jnp.bfloat16),
            pltpu.VMEM((half,) + packed, jnp.bfloat16),
            pltpu.VMEM((half,) + packed, jnp.bfloat16),
            pltpu.VMEM((outers,) + packed, jnp.bfloat16),
            pltpu.VMEM((rows, capacity), jnp.bfloat16),
            pltpu.VMEM((fits, rows, capacity), jnp.bfloat16),
            pltpu.VMEM((rows, width), jnp.float32),
            pltpu.VMEM((fits, rows, width), jnp.float32),
            dma((2,)),
            dma((heads,)),
            dma((heads,)),
            dma((groups,)),
            dma((groups,)),
            dma((groups,)),
            dma((groups,)),
            dma((groups,)),
            dma((groups,)),
            dma((half,)),
            dma((half,)),
            dma((half,)),
            dma((outers,)),
            dma((outers,)),
            dma((outers,)),
            dma((outers,)),
            dma((outers,)),
            dma((groups,)),
            dma((groups,)),
        ],
        compiler_params=pltpu.CompilerParams(collective_id=2, has_side_effects=True, **PARAMS),
    )(
        sizes,
        queries.reshape(layers * heads, width),
        keys[:, 0],
        values[:, 0],
        indices[0],
    )
    return pl.pallas_call(
        place_kernel,
        out_shape=jax.ShapeDtypeStruct((1, SLOTS, capacity, width), jnp.bfloat16),
        in_specs=[SMEM, VMEM, VMEM],
        out_specs=VMEM,
        compiler_params=pltpu.CompilerParams(**PARAMS),
    )(owners, probs, solved)


def solution(mesh):
    in_specs = (
        P(None, None, ("head", "seq"), None),
        P(None, "head", "seq", None),
        P(None, "head", "seq", None),
        P("head", None, None),
        P("head", None),
        P("head", None),
    )
    out_specs = P("head", "seq", None, None)
    return jax.shard_map(
        on_device, mesh=mesh, in_specs=in_specs, out_specs=out_specs, check_vma=False
    )
```

```python
import jax
import jax.numpy as jnp
from jax import lax
from jax.experimental import pallas as pl
from jax.experimental.pallas import tpu as pltpu
from jax.sharding import PartitionSpec as P

FITS_LAYER = 4
SLOTS = 3
RIDGE = 0.3
LANES = 128
FAR = -(2.0**100)
LOG2E = 1.4426950408889634
PAIR = 2
BAND = 32
PANEL = 8
STEP = 0.95
HOP = 2.55
SOLVE = 3.6

SUBLANES = 8
MESH = pl.DeviceIdType.MESH
NT = (((1,), (1,)), ((), ()))
TN = (((0,), (0,)), ((), ()))


def eliminate(system, target, first, last):
    rows = system.shape[0]
    row = lax.broadcasted_iota(jnp.int32, (rows, 1), 0)
    for begin in range(first, last, PANEL):
        size = min(PANEL, last - begin)
        columns = [
            jnp.broadcast_to(system[:, k : k + 1], (rows, LANES)) for k in range(begin, begin + size)
        ]
        for at in range(size):
            k = begin + at
            column = columns[at]
            inverse = 1.0 / column[k : k + 1]
            pivot_s = system[k : k + 1] * inverse
            pivot_t = target[k : k + 1] * inverse
            column = jnp.where(row == k, column - 1.0, column)
            for later in range(at + 1, size):
                columns[later] = columns[later] - column * (columns[later][k : k + 1] * inverse)
            system = system - column * pivot_s
            target = target - column * pivot_t
    return system, target


def solve_rows(system, target):
    rows = system.shape[0]
    row = lax.broadcasted_iota(jnp.int32, (rows, 1), 0)
    lane = lax.broadcasted_iota(jnp.int32, (1, rows), 1)

    def step(k, state):
        system, target = state
        column = jnp.sum(jnp.where(lane == k, system, 0.0), axis=1, keepdims=True)
        here = row == k
        inverse = 1.0 / jnp.sum(jnp.where(here, column, 0.0), axis=0, keepdims=True)
        pivot_s = jnp.sum(jnp.where(here, system, 0.0), axis=0, keepdims=True) * inverse
        pivot_t = jnp.sum(jnp.where(here, target, 0.0), axis=0, keepdims=True) * inverse
        column = jnp.where(here, column - 1.0, column)
        return system - column * pivot_s, target - column * pivot_t

    return lax.fori_loop(0, rows, step, (system, target))[1]


def top_of(tail):
    tail = tail.astype(jnp.float32)
    return tail[:, 0:1] + tail[:, 64:65]


def tail_of(top):
    lane = lax.broadcasted_iota(jnp.int32, (top.shape[0], LANES), 1)
    high = top.astype(jnp.bfloat16)
    low = (top - high.astype(jnp.float32)).astype(jnp.bfloat16)
    return jnp.where(lane < 64, high.astype(jnp.float32), low.astype(jnp.float32)).astype(
        jnp.bfloat16
    )


def others():
    heads, groups = lax.axis_size("head"), lax.axis_size("seq")
    my_head, me = lax.axis_index("head"), lax.axis_index("seq")
    for shift in range(heads):
        for step in range(groups):
            if shift or step:
                yield (
                    shift * groups + step,
                    lax.rem(my_head + shift, heads),
                    lax.rem(me + step, groups),
                )


def greet():
    barrier = pltpu.get_barrier_semaphore()
    for _, head, seq in others():
        pl.semaphore_signal(
            barrier, inc=1, device_id={"head": head, "seq": seq}, device_id_type=MESH
        )


def admit():
    pl.semaphore_wait(
        pltpu.get_barrier_semaphore(), lax.axis_size("head") * lax.axis_size("seq") - 1
    )


def send(source, target, send_sem, recv_sem, peer, head=None):
    return pltpu.make_async_remote_copy(
        src_ref=source,
        dst_ref=target,
        send_sem=send_sem,
        recv_sem=recv_sem,
        device_id={"seq": peer} if head is None else {"head": head, "seq": peer},
        device_id_type=MESH,
    )


def fit_kernel(
    sizes_hbm, owners_hbm, q_hbm, k_hbm, v_hbm, idx_hbm, p_ref, x_ref,
    sizes_ref, owners_ref, q_in, idx_ref,
    piece, table, k_ref, v_ref, s_ref, g_ref, high_ref, low_ref, t_ref,
    part, part_in, chunk_mine, chunks, gram_out, gram_in,
    e_out, e_in, pair, both, z_out, z_in, p_all, x_mine, x_all,
    load, send_q, recv_q, send_part, recv_part, send_chunk, recv_chunk, send_gram, recv_gram,
    send_e, recv_e, send_z, recv_z, send_p, recv_p, send_x, recv_x,
):
    layers, local_len, width = k_ref.shape
    fits, capacity = idx_ref.shape
    heads, my_head = lax.axis_size("head"), lax.axis_index("head")
    groups, me = lax.axis_size("seq"), lax.axis_index("seq")
    rows = groups * heads
    outer, inner = me // PAIR, lax.rem(me, PAIR)
    outers, half = groups // PAIR, fits // PAIR
    partner = outer * PAIR + 1 - inner
    fit_mine = jnp.minimum(me, fits - 1)
    chunk = layers * rows // groups
    start = me * local_len
    lane = lax.broadcasted_iota(jnp.int32, (rows, LANES), 1)
    near = (outer >= outers // 2).astype(jnp.int32)
    far = 1 - near
    inside_line = (outer > 0) & (outer < outers - 1)
    wide = gram_in.shape[2]
    middle = (rows + wide) // 2

    loads = [
        pltpu.make_async_copy(k_hbm, k_ref, load.at[0]),
        pltpu.make_async_copy(v_hbm, v_ref, load.at[1]),
        pltpu.make_async_copy(idx_hbm, idx_ref, load.at[2]),
        pltpu.make_async_copy(q_hbm, q_in, load.at[3]),
        pltpu.make_async_copy(sizes_hbm, sizes_ref, load.at[4]),
        pltpu.make_async_copy(owners_hbm, owners_ref, load.at[5]),
    ]
    loads[3].start()
    greet()
    for at in (4, 5, 2, 0, 1):
        loads[at].start()
    loads[3].wait()
    drawn_rows = q_in[...].astype(jnp.float32)
    for head in range(heads):
        for layer in range(layers):
            at = layer * heads + head
            piece[head, layer : layer + 1, :] = drawn_rows[at : at + 1]
    admit()
    my_row = me * heads + my_head
    asked = []
    for at, head, seq in others():
        asked.append(
            send(piece.at[head], table.at[my_row], send_q.at[at], recv_q.at[at], seq, head)
        )
        asked[-1].start()
    table[my_row] = piece[my_head]
    for copy in asked:
        copy.wait_recv()
    for at in (0, 2, 4, 5):
        loads[at].wait()
    for layer in range(layers):
        query_rows = table[:, layer, :].astype(jnp.bfloat16)
        s_ref[layer] = lax.dot_general(
            query_rows, k_ref[layer], NT, preferred_element_type=jnp.float32
        ) * (width ** (-0.5) * LOG2E)

    parts = [
        send(
            part.at[lax.rem(me + step, groups)], part_in.at[step],
            send_part.at[step], recv_part.at[step], lax.rem(me + step, groups),
        )
        for step in range(1, groups)
    ]

    def attend():
        loads[1].wait()
        for layer in range(layers):
            scores = s_ref[layer]
            peak = jnp.max(scores, axis=1, keepdims=True)
            weights = jnp.exp2(scores - peak)
            total = jnp.sum(weights, axis=1, keepdims=True)
            numer = jnp.dot(
                weights.astype(jnp.bfloat16), v_ref[layer], preferred_element_type=jnp.float32
            )
            side = jnp.where(lane < 64, total, peak)
            for at in range(rows // chunk):
                slot = layer * (rows // chunk) + at
                part[slot, 0] = numer[at * chunk : (at + 1) * chunk]
                part[slot, 1] = side[at * chunk : (at + 1) * chunk]
        for copy in parts:
            copy.start()
        part_in[0] = part[me]

    def produce(fit):
        layer = fit // FITS_LAYER
        size = sizes_ref[0, fit]
        offset = idx_ref[pl.ds(fit, 1), :] - start
        position = lax.broadcasted_iota(jnp.int32, (1, capacity), 1)
        inside = (offset >= 0) & (offset < local_len) & (position < size)
        high_ref[...] = jnp.broadcast_to(
            jnp.where(inside, offset >> 7, -1), (SUBLANES, capacity)
        )
        low_ref[...] = jnp.broadcast_to(offset & (LANES - 1), (SUBLANES, capacity))
        band = min(rows, BAND)

        def one_band(base_row):
            def one_tile(tile, top):
                base = pl.multiple_of(tile * LANES, LANES)
                high = high_ref[:, pl.ds(base, LANES)]
                low = low_ref[:, pl.ds(base, LANES)]
                picked = [jnp.full((SUBLANES, LANES), FAR, jnp.float32)] * (band // SUBLANES)
                for block in range(local_len // LANES):
                    here = high == block
                    for group in range(band // SUBLANES):
                        scored = s_ref[
                            layer,
                            pl.ds(base_row + group * SUBLANES, SUBLANES),
                            block * LANES : (block + 1) * LANES,
                        ]
                        found = jnp.take_along_axis(
                            scored, low, axis=1, mode="promise_in_bounds"
                        )
                        picked[group] = jnp.where(here, found, picked[group])
                joined = jnp.concatenate(picked, axis=0)
                g_ref[pl.ds(base_row, band), pl.ds(base, LANES)] = joined
                return jnp.maximum(top, joined)

            top = lax.fori_loop(
                0,
                capacity // LANES,
                one_tile,
                jnp.full((band, LANES), FAR, jnp.float32),
                unroll=True if rows == band else 1,
            )
            t_ref[pl.ds(base_row, band), :] = top

        if rows == band:
            one_band(0)
        else:

            def step(at, carry):
                one_band(pl.multiple_of(at * band, band))
                return carry

            lax.fori_loop(0, rows // band, step, 0)
        top = jnp.ceil(jnp.max(t_ref[...], axis=1, keepdims=True))
        picked = g_ref[...]
        return jnp.where(picked > 0.5 * FAR, jnp.exp2(picked - top), 0.0), top

    gram_lane = lax.broadcasted_iota(jnp.int32, (rows, wide), 1)

    def gram_copy(at, fit):
        return send(gram_out.at[at], gram_in.at[me], send_gram.at[at], recv_gram.at[me], fit)

    def fill_gram(at, expo, top):
        total = jnp.sum(expo.astype(jnp.float32), axis=1, keepdims=True)
        gram_out[at] = jnp.where(gram_lane >= middle, top, total)
        gram_out[at, :, :rows] = lax.dot_general(
            expo, expo, NT, preferred_element_type=jnp.float32
        )

    cut = capacity // 2
    spans = (slice(cut, capacity + LANES), slice(0, cut))
    plain = (slice(cut, capacity), slice(0, cut))
    gives = [j * PAIR + 1 - inner for j in range(half)]
    keeps = [j * PAIR + inner for j in range(half)]

    def cross(j, q):
        return send(
            e_out.at[j, :, spans[q]], e_in.at[j, :, spans[q]],
            send_e.at[j, q], recv_e.at[j, q], partner,
        )

    def stream(way, j, q):
        return send(
            z_out.at[way, j, :, spans[q]], z_in.at[way, j, :, spans[q]],
            send_z.at[way, j, q], recv_z.at[way, j, q],
            lax.rem(me + PAIR * (1 - 2 * way) + groups, groups),
        )

    def onward(j, q):
        return send(
            p_all.at[keeps[j], :, plain[q]], p_all.at[keeps[j], :, plain[q]],
            send_p.at[j, q], recv_p.at[j, q], partner,
        )

    def blend(one, other, at):
        first, second = top_of(one[:, capacity:]), top_of(other[:, capacity:])
        top = jnp.maximum(first, second)
        return (
            one[:, at] * jnp.exp2(first - top).astype(jnp.bfloat16)
            + other[:, at] * jnp.exp2(second - top).astype(jnp.bfloat16)
        ), top

    def put(ref, q, mixed):
        ref[:, plain[q]] = mixed[0]
        if q == 0:
            ref[:, capacity:] = tail_of(mixed[1])

    def give(j):
        expo, top = produce(gives[j])
        expo = expo.astype(jnp.bfloat16)
        e_out[j, :, :capacity] = expo
        e_out[j, :, capacity:] = tail_of(top)
        for q in range(2):
            cross(j, q).start()
        fill_gram(j, expo, top)
        gram_copy(j, gives[j]).start()

    def keep(j):
        expo, top = produce(keeps[j])
        expo = expo.astype(jnp.bfloat16)
        pair[j, :, :capacity] = expo
        pair[j, :, capacity:] = tail_of(top)
        fill_gram(half + j, expo, top)
        pl.when(keeps[j] != me)(gram_copy(half + j, keeps[j]).start)

    def join(j, q):
        cross(j, q).wait_recv()
        mixed = blend(pair.at[j], e_in.at[j], plain[q])
        put(both.at[j], q, mixed)

        @pl.when(~inside_line)
        def _():
            put(z_out.at[near, j], q, mixed)
            stream(near, j, q).start()

    def pass_near(j, q):

        @pl.when(inside_line)
        def _():
            stream(near, j, q).wait_recv()
            put(z_out.at[near, j], q, blend(both.at[j], z_in.at[near, j], plain[q]))
            stream(near, j, q).start()

    def pass_far(j, q):
        stream(far, j, q).wait_recv()

        @pl.when(inside_line)
        def _():
            put(z_out.at[far, j], q, blend(both.at[j], z_in.at[far, j], plain[q]))
            stream(far, j, q).start()

        p_all[keeps[j], :, plain[q]] = blend(z_out.at[near, j], z_in.at[far, j], plain[q])[0]
        onward(j, q).start()

    def merge_targets():
        for copy in parts:
            copy.wait_recv()
        peak = part_in[0, 1][:, 64:65]
        for step in range(1, groups):
            peak = jnp.maximum(peak, part_in[step, 1][:, 64:65])
        numer, total = 0.0, 0.0
        for step in range(groups):
            factor = jnp.exp2(part_in[step, 1][:, 64:65] - peak)
            numer = numer + part_in[step, 0] * factor
            total = total + part_in[step, 1][:, 0:1] * factor
        target = numer / total
        chunk_mine[...] = target
        chunks[me] = target
        for copy in spread:
            copy.start()

    spread = [
        send(
            chunk_mine, chunks.at[me], send_chunk.at[step], recv_chunk.at[step],
            lax.rem(me + step, groups),
        )
        for step in range(1, groups)
    ]
    results = [
        send(
            x_mine, x_all.at[fit_mine], send_x.at[step], recv_x.at[step],
            lax.rem(me + step, groups),
        )
        for step in range(1, groups)
    ]

    def only(condition, act):
        if groups == fits:
            act()
        else:
            pl.when(condition)(act)

    def gather_system():
        for copy in spread:
            copy.wait_recv()

        def wait_grams():
            for step in range(1, groups):
                source = lax.rem(me + step, groups)
                send(
                    gram_out.at[0], gram_in.at[source], send_gram.at[0], recv_gram.at[source], source
                ).wait_recv()

        only(me < fits, wait_grams)

    state = {}

    def assemble():
        diagonal = lax.broadcasted_iota(jnp.int32, (rows, wide), 0) == lax.broadcasted_iota(
            jnp.int32, (rows, wide), 1
        )

        def across_lanes(column):
            return jnp.sum(jnp.where(diagonal, column, 0.0), axis=0, keepdims=True)

        gram_in[me] = gram_out[half + jnp.minimum(outer, half - 1)]
        tops = [gram_in[source, :, middle : middle + 1] for source in range(groups)]
        top = tops[0]
        for other in tops[1:]:
            top = jnp.maximum(top, other)
        gram, total = 0.0, 0.0
        for source in range(groups):
            factor = jnp.exp2(tops[source] - top)
            total = total + factor * gram_in[source, :, rows : rows + 1]
            gram = gram + gram_in[source] * factor * across_lanes(factor)
        scale = 1.0 / total
        gram = jnp.where(gram_lane < rows, gram * scale * across_lanes(scale), 0.0)
        trace = jnp.sum(jnp.where(diagonal, gram, 0.0))
        ridge = RIDGE * trace / sizes_ref[0, fit_mine].astype(jnp.float32)
        span = rows // chunk
        base = (fit_mine // FITS_LAYER) * span
        target = jnp.concatenate([chunks[base + at] for at in range(span)], axis=0)
        state["target"] = target.astype(jnp.bfloat16).astype(jnp.float32)
        state["system"] = jnp.where(diagonal, gram + ridge, gram)
        state["scale"] = scale

    def conclude(solved):
        solved = solved * state["scale"]
        x_mine[...] = solved
        x_all[fit_mine] = solved
        for copy in results:
            copy.start()

    small = rows <= 64 and groups == fits

    def solve_first():
        gather_system()
        if small:
            assemble()
            state["system"], state["target"] = eliminate(
                state["system"], state["target"], 0, rows // 2
            )

    def solve_last():
        if small:
            conclude(eliminate(state["system"], state["target"], rows // 2, rows)[1])
        else:

            def whole():
                assemble()
                conclude(solve_rows(state["system"][:, :rows], state["target"]))

            only(me < fits, whole)

    agenda = [(1.54, attend, ()), (4.65, merge_targets, ())]
    agenda += [(10.23, solve_first, ()), (10.7, solve_last, ())]
    for j in range(half):
        agenda += [(1.62 * j, give, (j,)), (3.0 + 1.22 * j, keep, (j,))]
        for q in range(2):
            at = 3.42 + 1.17 * j + 0.4 * q
            agenda.append((at, join, (j, q)))
            agenda.append((at + 2.16, pass_near, (j, q)))
            agenda.append((at + 4.75, pass_far, (j, q)))
    for _, act, at in sorted(agenda, key=lambda entry: entry[0]):
        act(*at)
    halves = [(j, q) for j in range(half) for q in range(2)]
    for copy in asked + parts + spread:
        copy.wait_send()
    for j, q in halves:
        cross(j, q).wait_send()
        onward(j, q).wait_send()
    for at, fit in enumerate(gives + keeps):
        if at < half:
            gram_copy(at, fit).wait_send()
        else:
            pl.when(fit != me)(gram_copy(at, fit).wait_send)
    for j, q in halves:
        stream(near, j, q).wait_send()
        pl.when(inside_line)(stream(far, j, q).wait_send)
    for j, q in halves:
        onward(j, q).wait_recv()
    for step in range(1, groups):
        source = lax.rem(me + groups - step, groups)
        only(source < fits, results[step - 1].wait_recv)
        only(me < fits, results[step - 1].wait_send)
    count = jnp.int32(0)
    chosen = [jnp.int32(0)] * SLOTS
    for fit in range(fits):
        mine = owners_ref[0, fit] == me
        for slot in range(SLOTS):
            chosen[slot] = jnp.where(mine & (count == slot), fit, chosen[slot])
        count = count + mine.astype(jnp.int32)
    for slot in range(SLOTS):
        p_ref[slot] = p_all[chosen[slot]]
        x_ref[slot] = jnp.where(count > slot, x_all[chosen[slot]], 0.0)


def place_kernel(p_ref, x_ref, out_hbm, out_ref, store):
    stores = []
    for slot in range(SLOTS):
        probs = p_ref[slot]
        rows = x_ref[slot]
        high = rows.astype(jnp.bfloat16)
        low = (rows - high.astype(jnp.float32)).astype(jnp.bfloat16)
        out_ref[slot] = lax.dot_general(
            jnp.concatenate([probs, probs], axis=0),
            jnp.concatenate([high, low], axis=0),
            TN,
            preferred_element_type=jnp.float32,
        ).astype(jnp.bfloat16)
        stores.append(pltpu.make_async_copy(out_ref.at[slot], out_hbm.at[0, slot], store.at[slot]))
        stores[-1].start()
    for copy in stores:
        copy.wait()


VMEM = pl.BlockSpec(memory_space=pltpu.VMEM)
ANY = pl.BlockSpec(memory_space=pl.ANY)


def on_device(queries, keys, values, indices, sizes, owners):
    layers, heads, count, width = queries.shape
    groups = lax.axis_size("seq")
    rows = groups * heads * count
    local_len = keys.shape[2]
    fits, capacity = indices.shape[1:]
    dma = pltpu.SemaphoreType.DMA
    params = dict(vmem_limit_bytes=(24 + rows // 8) * 1024 * 1024)
    half = fits // PAIR
    chunk = layers * rows // groups
    wide = (rows // LANES + 1) * LANES
    packed = (rows, capacity + LANES)
    probs, solved = pl.pallas_call(
        fit_kernel,
        out_shape=(
            jax.ShapeDtypeStruct((SLOTS, rows, capacity), jnp.bfloat16),
            jax.ShapeDtypeStruct((SLOTS, rows, width), jnp.float32),
        ),
        in_specs=[ANY] * 6,
        out_specs=(VMEM, VMEM),
        scratch_shapes=[
            pltpu.SMEM((1, fits), jnp.int32),
            pltpu.SMEM((1, fits), jnp.int32),
            pltpu.VMEM((layers * heads, width), queries.dtype),
            pltpu.VMEM((fits, capacity), jnp.int32),
            pltpu.VMEM((heads, layers, width), jnp.float32),
            pltpu.VMEM((rows, layers, width), jnp.float32),
            pltpu.VMEM((layers, local_len, width), jnp.bfloat16),
            pltpu.VMEM((layers, local_len, width), jnp.bfloat16),
            pltpu.VMEM((layers, rows, local_len), jnp.float32),
            pltpu.VMEM((rows, capacity), jnp.float32),
            pltpu.VMEM((SUBLANES, capacity), jnp.int32),
            pltpu.VMEM((SUBLANES, capacity), jnp.int32),
            pltpu.VMEM((rows, LANES), jnp.float32),
            pltpu.VMEM((groups, 2, chunk, width), jnp.float32),
            pltpu.VMEM((groups, 2, chunk, width), jnp.float32),
            pltpu.VMEM((chunk, width), jnp.float32),
            pltpu.VMEM((groups, chunk, width), jnp.float32),
            pltpu.VMEM((fits, rows, wide), jnp.float32),
            pltpu.VMEM((groups, rows, wide), jnp.float32),
            pltpu.VMEM((half,) + packed, jnp.bfloat16),
            pltpu.VMEM((half,) + packed, jnp.bfloat16),
            pltpu.VMEM((half,) + packed, jnp.bfloat16),
            pltpu.VMEM((half,) + packed, jnp.bfloat16),
            pltpu.VMEM((2, half) + packed, jnp.bfloat16),
            pltpu.VMEM((2, half) + packed, jnp.bfloat16),
            pltpu.VMEM((fits, rows, capacity), jnp.bfloat16),
            pltpu.VMEM((rows, width), jnp.float32),
            pltpu.VMEM((fits, rows, width), jnp.float32),
            dma((6,)),
            dma((heads * groups,)),
            dma((heads * groups,)),
            dma((groups,)),
            dma((groups,)),
            dma((groups,)),
            dma((groups,)),
            dma((fits,)),
            dma((groups,)),
            dma((half, 2)),
            dma((half, 2)),
            dma((2, half, 2)),
            dma((2, half, 2)),
            dma((half, 2)),
            dma((half, 2)),
            dma((groups,)),
            dma((groups,)),
        ],
        compiler_params=pltpu.CompilerParams(collective_id=2, has_side_effects=True, **params),
    )(
        *(
            pltpu.with_memory_space_constraint(array, pltpu.HBM)
            for array in (
                sizes,
                owners,
                queries.reshape(layers * heads, width),
                keys[:, 0],
                values[:, 0],
                indices[0],
            )
        )
    )
    return pl.pallas_call(
        place_kernel,
        out_shape=jax.ShapeDtypeStruct((1, SLOTS, capacity, width), jnp.bfloat16),
        in_specs=[VMEM, VMEM],
        out_specs=ANY,
        scratch_shapes=[pltpu.VMEM((SLOTS, capacity, width), jnp.bfloat16), dma((SLOTS,))],
        compiler_params=pltpu.CompilerParams(**params),
    )(probs, solved)


def solution(mesh):
    in_specs = (
        P(None, None, ("head", "seq"), None),
        P(None, "head", "seq", None),
        P(None, "head", "seq", None),
        P("head", None, None),
        P("head", None),
        P("head", None),
    )
    out_specs = P("head", "seq", None, None)
    return jax.shard_map(
        on_device, mesh=mesh, in_specs=in_specs, out_specs=out_specs, check_vma=False
    )
```

```python
import jax
import jax.numpy as jnp
from jax import lax
from jax.experimental import pallas as pl
from jax.experimental.pallas import tpu as pltpu
from jax.sharding import PartitionSpec as P

FITS_LAYER = 4
SLOTS = 3
RIDGE = 0.3
LANES = 128
FAR = -(2.0**100)
LOG2E = 1.4426950408889634
PAIR = 2
BAND = 32
COARSE = 8.0
PANEL = 8
STEP = 0.95
HOP = 2.55
SOLVE = 3.6

SUBLANES = 8
MESH = pl.DeviceIdType.MESH
NT = (((1,), (1,)), ((), ()))
TN = (((0,), (0,)), ((), ()))


def eliminate(system, target, first, last):
    rows = system.shape[0]
    row = lax.broadcasted_iota(jnp.int32, (rows, 1), 0)
    for begin in range(first, last, PANEL):
        size = min(PANEL, last - begin)
        columns = [
            jnp.broadcast_to(system[:, k : k + 1], (rows, LANES)) for k in range(begin, begin + size)
        ]
        for at in range(size):
            k = begin + at
            column = columns[at]
            inverse = 1.0 / column[k : k + 1]
            pivot_s = system[k : k + 1] * inverse
            pivot_t = target[k : k + 1] * inverse
            column = jnp.where(row == k, column - 1.0, column)
            for later in range(at + 1, size):
                columns[later] = columns[later] - column * (columns[later][k : k + 1] * inverse)
            system = system - column * pivot_s
            target = target - column * pivot_t
    return system, target


def solve_rows(system, target):
    rows = system.shape[0]
    row = lax.broadcasted_iota(jnp.int32, (rows, 1), 0)
    lane = lax.broadcasted_iota(jnp.int32, (1, rows), 1)

    def step(k, state):
        system, target = state
        column = jnp.sum(jnp.where(lane == k, system, 0.0), axis=1, keepdims=True)
        here = row == k
        inverse = 1.0 / jnp.sum(jnp.where(here, column, 0.0), axis=0, keepdims=True)
        pivot_s = jnp.sum(jnp.where(here, system, 0.0), axis=0, keepdims=True) * inverse
        pivot_t = jnp.sum(jnp.where(here, target, 0.0), axis=0, keepdims=True) * inverse
        column = jnp.where(here, column - 1.0, column)
        return system - column * pivot_s, target - column * pivot_t

    return lax.fori_loop(0, rows, step, (system, target))[1]


def others():
    heads, groups = lax.axis_size("head"), lax.axis_size("seq")
    my_head, me = lax.axis_index("head"), lax.axis_index("seq")
    for shift in range(heads):
        for step in range(groups):
            if shift or step:
                yield (
                    shift * groups + step,
                    lax.rem(my_head + shift, heads),
                    lax.rem(me + step, groups),
                )


def greet():
    barrier = pltpu.get_barrier_semaphore()
    for _, head, seq in others():
        pl.semaphore_signal(
            barrier, inc=1, device_id={"head": head, "seq": seq}, device_id_type=MESH
        )


def admit():
    pl.semaphore_wait(
        pltpu.get_barrier_semaphore(), lax.axis_size("head") * lax.axis_size("seq") - 1
    )


def send(source, target, send_sem, recv_sem, peer, head=None):
    return pltpu.make_async_remote_copy(
        src_ref=source,
        dst_ref=target,
        send_sem=send_sem,
        recv_sem=recv_sem,
        device_id={"seq": peer} if head is None else {"head": head, "seq": peer},
        device_id_type=MESH,
    )


def fit_kernel(
    sizes_hbm, owners_hbm, q_hbm, k_hbm, v_hbm, idx_hbm, p_ref, x_ref,
    sizes_ref, owners_ref, q_in, idx_ref,
    piece, table, k_ref, v_ref, s_ref, g_ref, high_ref, low_ref, t_ref,
    part, part_in, chunk_mine, chunks, gram_out, gram_in,
    e_out, e_in, pair, both, z_out, z_in, p_all, x_mine, x_all,
    load, send_q, recv_q, send_part, recv_part, send_chunk, recv_chunk, send_gram, recv_gram,
    send_e, recv_e, send_z, recv_z, send_p, recv_p, send_x, recv_x,
):
    layers, local_len, width = k_ref.shape
    fits, capacity = idx_ref.shape
    heads, my_head = lax.axis_size("head"), lax.axis_index("head")
    groups, me = lax.axis_size("seq"), lax.axis_index("seq")
    rows = groups * heads
    outer, inner = me // PAIR, lax.rem(me, PAIR)
    outers, half = groups // PAIR, fits // PAIR
    partner = outer * PAIR + 1 - inner
    fit_mine = jnp.minimum(me, fits - 1)
    chunk = layers * rows // groups
    start = me * local_len
    lane = lax.broadcasted_iota(jnp.int32, (rows, LANES), 1)
    near = (outer >= outers // 2).astype(jnp.int32)
    far = 1 - near
    inside_line = (outer > 0) & (outer < outers - 1)
    wide = gram_in.shape[2]
    middle = (rows + wide) // 2

    loads = [
        pltpu.make_async_copy(k_hbm, k_ref, load.at[0]),
        pltpu.make_async_copy(v_hbm, v_ref, load.at[1]),
        pltpu.make_async_copy(idx_hbm, idx_ref, load.at[2]),
        pltpu.make_async_copy(q_hbm, q_in, load.at[3]),
        pltpu.make_async_copy(sizes_hbm, sizes_ref, load.at[4]),
        pltpu.make_async_copy(owners_hbm, owners_ref, load.at[5]),
    ]
    loads[3].start()
    greet()
    for at in (4, 5, 2, 0, 1):
        loads[at].start()
    loads[3].wait()
    drawn_rows = q_in[...].astype(jnp.float32)
    for head in range(heads):
        for layer in range(layers):
            at = layer * heads + head
            piece[head, layer : layer + 1, :] = drawn_rows[at : at + 1]
    admit()
    my_row = me * heads + my_head
    asked = []
    for at, head, seq in others():
        asked.append(
            send(piece.at[head], table.at[my_row], send_q, recv_q, seq, head)
        )
        asked[-1].start()
    table[my_row] = piece[my_head]
    every = table.at[pl.ds(0, heads * groups - 1)]
    send(every, every, send_q, recv_q, partner).wait_recv()
    for at in (0, 2, 4, 5):
        loads[at].wait()
    for layer in range(layers):
        query_rows = table[:, layer, :].astype(jnp.bfloat16)
        s_ref[layer] = lax.dot_general(
            query_rows, k_ref[layer], NT, preferred_element_type=jnp.float32
        ) * (width ** (-0.5) * LOG2E)

    parts = [
        send(
            part.at[lax.rem(me + step, groups)], part_in.at[step],
            send_part, recv_part, lax.rem(me + step, groups),
        )
        for step in range(1, groups)
    ]

    def attend():
        loads[1].wait()
        for layer in range(layers):
            scores = s_ref[layer]
            peak = jnp.max(scores, axis=1, keepdims=True)
            weights = jnp.exp2(scores - peak)
            total = jnp.sum(weights, axis=1, keepdims=True)
            numer = jnp.dot(
                weights.astype(jnp.bfloat16), v_ref[layer], preferred_element_type=jnp.float32
            )
            side = jnp.where(lane < 64, total, peak)
            for at in range(rows // chunk):
                slot = layer * (rows // chunk) + at
                part[slot, 0] = numer[at * chunk : (at + 1) * chunk]
                part[slot, 1] = side[at * chunk : (at + 1) * chunk]
        for copy in parts:
            copy.start()
        part_in[0] = part[me]

    def produce(fit):
        layer = fit // FITS_LAYER
        size = sizes_ref[0, fit]
        offset = idx_ref[pl.ds(fit, 1), :] - start
        position = lax.broadcasted_iota(jnp.int32, (1, capacity), 1)
        inside = (offset >= 0) & (offset < local_len) & (position < size)
        high_ref[...] = jnp.broadcast_to(
            jnp.where(inside, offset >> 7, -1), (SUBLANES, capacity)
        )
        low_ref[...] = jnp.broadcast_to(offset & (LANES - 1), (SUBLANES, capacity))
        band = min(rows, BAND)

        def one_band(base_row):
            def one_tile(tile, top):
                base = pl.multiple_of(tile * LANES, LANES)
                high = high_ref[:, pl.ds(base, LANES)]
                low = low_ref[:, pl.ds(base, LANES)]
                picked = [jnp.full((SUBLANES, LANES), FAR, jnp.float32)] * (band // SUBLANES)
                for block in range(local_len // LANES):
                    here = high == block
                    for group in range(band // SUBLANES):
                        scored = s_ref[
                            layer,
                            pl.ds(base_row + group * SUBLANES, SUBLANES),
                            block * LANES : (block + 1) * LANES,
                        ]
                        found = jnp.take_along_axis(
                            scored, low, axis=1, mode="promise_in_bounds"
                        )
                        picked[group] = jnp.where(here, found, picked[group])
                joined = jnp.concatenate(picked, axis=0)
                g_ref[pl.ds(base_row, band), pl.ds(base, LANES)] = joined
                return jnp.maximum(top, joined)

            top = lax.fori_loop(
                0,
                capacity // LANES,
                one_tile,
                jnp.full((band, LANES), FAR, jnp.float32),
                unroll=True if rows == band else 1,
            )
            t_ref[pl.ds(base_row, band), :] = top

        if rows == band:
            one_band(0)
        else:

            def step(at, carry):
                one_band(pl.multiple_of(at * band, band))
                return carry

            lax.fori_loop(0, rows // band, step, 0)
        top = COARSE * jnp.ceil(jnp.max(t_ref[...], axis=1, keepdims=True) * (1.0 / COARSE))
        picked = g_ref[...]
        return jnp.where(picked > 0.5 * FAR, jnp.exp2(picked - top), 0.0), top

    gram_lane = lax.broadcasted_iota(jnp.int32, (rows, wide), 1)

    def gram_copy(at, fit):
        return send(gram_out.at[at], gram_in.at[me], send_gram, recv_gram, fit)

    def fill_gram(at, expo, top):
        total = jnp.sum(expo.astype(jnp.float32), axis=1, keepdims=True)
        gram_out[at] = jnp.where(gram_lane >= middle, top, total)
        gram_out[at, :, :rows] = lax.dot_general(
            expo, expo, NT, preferred_element_type=jnp.float32
        )

    cut = capacity // 2
    spans = (slice(cut, capacity + LANES), slice(0, cut))
    plain = (slice(cut, capacity), slice(0, cut))
    gives = [j * PAIR + 1 - inner for j in range(half)]
    keeps = [j * PAIR + inner for j in range(half)]

    def cross(j, q):
        return send(
            e_out.at[j, :, spans[q]], e_in.at[j, :, spans[q]],
            send_e, recv_e.at[j, q], partner,
        )

    def stream(way, j, q):
        return send(
            z_out.at[way, j, :, spans[q]], z_in.at[way, j, :, spans[q]],
            send_z.at[way], recv_z.at[way, j, q],
            lax.rem(me + PAIR * (1 - 2 * way) + groups, groups),
        )

    def onward(j, q):
        return send(
            p_all.at[keeps[j], :, plain[q]], p_all.at[keeps[j], :, plain[q]],
            send_p, recv_p, partner,
        )

    def sent(ref, sem):
        send(ref, ref, sem, sem, partner).wait_send()

    def came(ref, sem):
        send(ref, ref, sem, sem, partner).wait_recv()

    def scales(one, other):
        first = one[:, capacity:].astype(jnp.float32)
        second = other[:, capacity:].astype(jnp.float32)
        top = jnp.maximum(first, second)
        wide_by = cut // LANES
        return (
            top.astype(jnp.bfloat16),
            jnp.concatenate([jnp.exp2(first - top).astype(jnp.bfloat16)] * wide_by, axis=1),
            jnp.concatenate([jnp.exp2(second - top).astype(jnp.bfloat16)] * wide_by, axis=1),
        )

    def blend(one, other, at):
        top, first, second = scales(one, other)
        return one[:, at] * first + other[:, at] * second, top

    def put(ref, q, mixed):
        ref[:, plain[q]] = mixed[0]
        if q == 0:
            ref[:, capacity:] = mixed[1]

    def tail_of(top):
        return jnp.broadcast_to(top, (rows, LANES)).astype(jnp.bfloat16)

    def give(j):
        expo, top = produce(gives[j])
        expo = expo.astype(jnp.bfloat16)
        e_out[j, :, :capacity] = expo
        e_out[j, :, capacity:] = tail_of(top)
        for q in range(2):
            cross(j, q).start()
        fill_gram(j, expo, top)
        gram_copy(j, gives[j]).start()

    def keep(j):
        expo, top = produce(keeps[j])
        expo = expo.astype(jnp.bfloat16)
        pair[j, :, :capacity] = expo
        pair[j, :, capacity:] = tail_of(top)
        fill_gram(half + j, expo, top)
        pl.when(keeps[j] != me)(gram_copy(half + j, keeps[j]).start)

    def join(j, q):
        cross(j, q).wait_recv()
        mixed = blend(pair.at[j], e_in.at[j], plain[q])
        put(both.at[j], q, mixed)

        @pl.when(~inside_line)
        def _():
            put(z_out.at[near, j], q, mixed)
            stream(near, j, q).start()

    def pass_near(j, q):

        @pl.when(inside_line)
        def _():
            stream(near, j, q).wait_recv()
            put(z_out.at[near, j], q, blend(both.at[j], z_in.at[near, j], plain[q]))
            stream(near, j, q).start()

    def pass_far(j, q):
        stream(far, j, q).wait_recv()

        @pl.when(inside_line)
        def _():
            put(z_out.at[far, j], q, blend(both.at[j], z_in.at[far, j], plain[q]))
            stream(far, j, q).start()

        p_all[keeps[j], :, plain[q]] = blend(z_out.at[near, j], z_in.at[far, j], plain[q])[0]
        onward(j, q).start()

    def merge_targets():
        came(part_in.at[pl.ds(1, groups - 1)], recv_part)
        peak = part_in[0, 1][:, 64:65]
        for step in range(1, groups):
            peak = jnp.maximum(peak, part_in[step, 1][:, 64:65])
        numer, total = 0.0, 0.0
        for step in range(groups):
            factor = jnp.exp2(part_in[step, 1][:, 64:65] - peak)
            numer = numer + part_in[step, 0] * factor
            total = total + part_in[step, 1][:, 0:1] * factor
        target = numer / total
        chunk_mine[...] = target
        chunks[me] = target
        for copy in spread:
            copy.start()

    spread = [
        send(
            chunk_mine, chunks.at[me], send_chunk, recv_chunk,
            lax.rem(me + step, groups),
        )
        for step in range(1, groups)
    ]
    results = [
        send(
            x_mine, x_all.at[fit_mine], send_x, recv_x,
            lax.rem(me + step, groups),
        )
        for step in range(1, groups)
    ]

    def only(condition, act):
        if groups == fits:
            act()
        else:
            pl.when(condition)(act)

    def gather_system():
        came(chunks.at[pl.ds(0, groups - 1)], recv_chunk)

        def wait_grams():
            came(gram_in.at[pl.ds(0, groups - 1)], recv_gram)

        only(me < fits, wait_grams)

    state = {}

    def assemble():
        diagonal = lax.broadcasted_iota(jnp.int32, (rows, wide), 0) == lax.broadcasted_iota(
            jnp.int32, (rows, wide), 1
        )

        def across_lanes(column):
            return jnp.sum(jnp.where(diagonal, column, 0.0), axis=0, keepdims=True)

        gram_in[me] = gram_out[half + jnp.minimum(outer, half - 1)]
        tops = [gram_in[source, :, middle : middle + 1] for source in range(groups)]
        top = tops[0]
        for other in tops[1:]:
            top = jnp.maximum(top, other)
        gram, total = 0.0, 0.0
        for source in range(groups):
            factor = jnp.exp2(tops[source] - top)
            total = total + factor * gram_in[source, :, rows : rows + 1]
            gram = gram + gram_in[source] * factor * across_lanes(factor)
        scale = 1.0 / total
        gram = jnp.where(gram_lane < rows, gram * scale * across_lanes(scale), 0.0)
        trace = jnp.sum(jnp.where(diagonal, gram, 0.0))
        ridge = RIDGE * trace / sizes_ref[0, fit_mine].astype(jnp.float32)
        span = rows // chunk
        base = (fit_mine // FITS_LAYER) * span
        target = jnp.concatenate([chunks[base + at] for at in range(span)], axis=0)
        state["target"] = target.astype(jnp.bfloat16).astype(jnp.float32)
        state["system"] = jnp.where(diagonal, gram + ridge, gram)
        state["scale"] = scale

    def conclude(solved):
        solved = solved * state["scale"]
        x_mine[...] = solved
        x_all[fit_mine] = solved
        for copy in results:
            copy.start()

    small = rows <= 64 and groups == fits

    def solve_first():
        gather_system()
        if small:
            assemble()
            state["system"], state["target"] = eliminate(
                state["system"], state["target"], 0, rows // 2
            )

    def solve_last():
        if small:
            conclude(eliminate(state["system"], state["target"], rows // 2, rows)[1])
        else:

            def whole():
                assemble()
                conclude(solve_rows(state["system"][:, :rows], state["target"]))

            only(me < fits, whole)

    agenda = [(1.54, attend, ()), (4.65, merge_targets, ())]
    agenda += [(10.23, solve_first, ()), (10.7, solve_last, ())]
    for j in range(half):
        agenda += [(1.62 * j, give, (j,)), (3.0 + 1.22 * j, keep, (j,))]
        for q in range(2):
            at = 3.42 + 1.17 * j + 0.4 * q
            agenda.append((at, join, (j, q)))
            agenda.append((at + 2.16, pass_near, (j, q)))
            agenda.append((at + 4.75, pass_far, (j, q)))
    for _, act, at in sorted(agenda, key=lambda entry: entry[0]):
        act(*at)
    sent(table.at[pl.ds(0, heads * groups - 1)], send_q)
    sent(part.at[pl.ds(0, groups - 1)], send_part)
    sent(chunks.at[pl.ds(0, groups - 1)], send_chunk)
    sent(e_out, send_e)
    if groups == fits:
        sent(gram_out.at[pl.ds(0, fits - 1)], send_gram)
    else:
        pl.when(me < fits)(lambda: sent(gram_out.at[pl.ds(0, fits - 1)], send_gram))
        pl.when(me >= fits)(lambda: sent(gram_out, send_gram))
    sent(z_out.at[near], send_z.at[near])
    pl.when(inside_line)(lambda: sent(z_out.at[far], send_z.at[far]))
    sent(p_all.at[pl.ds(0, half)], send_p)
    if groups == fits:
        came(x_all.at[pl.ds(0, fits - 1)], recv_x)
        sent(gram_in.at[pl.ds(0, groups - 1), :, :width], send_x)
    else:
        pl.when(me < fits)(lambda: came(x_all.at[pl.ds(0, fits - 1)], recv_x))
        pl.when(me < fits)(lambda: sent(gram_in.at[pl.ds(0, groups - 1), :, :width], send_x))
        pl.when(me >= fits)(lambda: came(x_all, recv_x))
    came(p_all.at[pl.ds(0, half)], recv_p)
    count = jnp.int32(0)
    chosen = [jnp.int32(0)] * SLOTS
    for fit in range(fits):
        mine = owners_ref[0, fit] == me
        for slot in range(SLOTS):
            chosen[slot] = jnp.where(mine & (count == slot), fit, chosen[slot])
        count = count + mine.astype(jnp.int32)
    for slot in range(SLOTS):
        p_ref[slot] = p_all[chosen[slot]]
        x_ref[slot] = jnp.where(count > slot, x_all[chosen[slot]], 0.0)


def place_kernel(p_ref, x_ref, out_hbm, out_ref, store):
    stores = []
    for slot in range(SLOTS):
        probs = p_ref[slot]
        rows = x_ref[slot]
        high = rows.astype(jnp.bfloat16)
        low = (rows - high.astype(jnp.float32)).astype(jnp.bfloat16)
        out_ref[slot] = lax.dot_general(
            jnp.concatenate([probs, probs], axis=0),
            jnp.concatenate([high, low], axis=0),
            TN,
            preferred_element_type=jnp.float32,
        ).astype(jnp.bfloat16)
        stores.append(pltpu.make_async_copy(out_ref.at[slot], out_hbm.at[0, slot], store.at[slot]))
        stores[-1].start()
    for copy in stores:
        copy.wait()


VMEM = pl.BlockSpec(memory_space=pltpu.VMEM)
ANY = pl.BlockSpec(memory_space=pl.ANY)


def on_device(queries, keys, values, indices, sizes, owners):
    layers, heads, count, width = queries.shape
    groups = lax.axis_size("seq")
    rows = groups * heads * count
    local_len = keys.shape[2]
    fits, capacity = indices.shape[1:]
    dma = pltpu.SemaphoreType.DMA
    params = dict(vmem_limit_bytes=(24 + rows // 8) * 1024 * 1024)
    half = fits // PAIR
    chunk = layers * rows // groups
    wide = (rows // LANES + 1) * LANES
    packed = (rows, capacity + LANES)
    probs, solved = pl.pallas_call(
        fit_kernel,
        out_shape=(
            jax.ShapeDtypeStruct((SLOTS, rows, capacity), jnp.bfloat16),
            jax.ShapeDtypeStruct((SLOTS, rows, width), jnp.float32),
        ),
        in_specs=[ANY] * 6,
        out_specs=(VMEM, VMEM),
        scratch_shapes=[
            pltpu.SMEM((1, fits), jnp.int32),
            pltpu.SMEM((1, fits), jnp.int32),
            pltpu.VMEM((layers * heads, width), queries.dtype),
            pltpu.VMEM((fits, capacity), jnp.int32),
            pltpu.VMEM((heads, layers, width), jnp.float32),
            pltpu.VMEM((rows, layers, width), jnp.float32),
            pltpu.VMEM((layers, local_len, width), jnp.bfloat16),
            pltpu.VMEM((layers, local_len, width), jnp.bfloat16),
            pltpu.VMEM((layers, rows, local_len), jnp.float32),
            pltpu.VMEM((rows, capacity), jnp.float32),
            pltpu.VMEM((SUBLANES, capacity), jnp.int32),
            pltpu.VMEM((SUBLANES, capacity), jnp.int32),
            pltpu.VMEM((rows, LANES), jnp.float32),
            pltpu.VMEM((groups, 2, chunk, width), jnp.float32),
            pltpu.VMEM((groups, 2, chunk, width), jnp.float32),
            pltpu.VMEM((chunk, width), jnp.float32),
            pltpu.VMEM((groups, chunk, width), jnp.float32),
            pltpu.VMEM((fits, rows, wide), jnp.float32),
            pltpu.VMEM((groups, rows, wide), jnp.float32),
            pltpu.VMEM((half,) + packed, jnp.bfloat16),
            pltpu.VMEM((half,) + packed, jnp.bfloat16),
            pltpu.VMEM((half,) + packed, jnp.bfloat16),
            pltpu.VMEM((half,) + packed, jnp.bfloat16),
            pltpu.VMEM((2, half) + packed, jnp.bfloat16),
            pltpu.VMEM((2, half) + packed, jnp.bfloat16),
            pltpu.VMEM((fits, rows, capacity), jnp.bfloat16),
            pltpu.VMEM((rows, width), jnp.float32),
            pltpu.VMEM((fits, rows, width), jnp.float32),
            dma((6,)),
            dma,
            dma,
            dma,
            dma,
            dma,
            dma,
            dma,
            dma,
            dma,
            dma((half, 2)),
            dma((2,)),
            dma((2, half, 2)),
            dma,
            dma,
            dma,
            dma,
        ],
        compiler_params=pltpu.CompilerParams(collective_id=2, has_side_effects=True, **params),
    )(
        *(
            pltpu.with_memory_space_constraint(array, pltpu.HBM)
            for array in (
                sizes,
                owners,
                queries.reshape(layers * heads, width),
                keys[:, 0],
                values[:, 0],
                indices[0],
            )
        )
    )
    return pl.pallas_call(
        place_kernel,
        out_shape=jax.ShapeDtypeStruct((1, SLOTS, capacity, width), jnp.bfloat16),
        in_specs=[VMEM, VMEM],
        out_specs=ANY,
        scratch_shapes=[pltpu.VMEM((SLOTS, capacity, width), jnp.bfloat16), dma((SLOTS,))],
        compiler_params=pltpu.CompilerParams(**params),
    )(probs, solved)


def solution(mesh):
    in_specs = (
        P(None, None, ("head", "seq"), None),
        P(None, "head", "seq", None),
        P(None, "head", "seq", None),
        P("head", None, None),
        P("head", None),
        P("head", None),
    )
    out_specs = P("head", "seq", None, None)
    return jax.shard_map(
        on_device, mesh=mesh, in_specs=in_specs, out_specs=out_specs, check_vma=False
    )
```

```python
import jax
import jax.numpy as jnp
from jax import lax
from jax.experimental import pallas as pl
from jax.experimental.pallas import tpu as pltpu
from jax.sharding import PartitionSpec as P

FITS_LAYER = 4
SLOTS = 3
RIDGE = 0.3
LANES = 128
FAR = -(2.0**100)
LOG2E = 1.4426950408889634
PAIR = 2
BAND = 32
COARSE = 8.0
PANEL = 8
STEP = 0.95
HOP = 2.55
SOLVE = 3.6

SUBLANES = 8
MESH = pl.DeviceIdType.MESH
NT = (((1,), (1,)), ((), ()))
TN = (((0,), (0,)), ((), ()))


def eliminate(system, target, first, last):
    rows = system.shape[0]
    row = lax.broadcasted_iota(jnp.int32, (rows, 1), 0)
    for begin in range(first, last, PANEL):
        size = min(PANEL, last - begin)
        columns = [
            jnp.broadcast_to(system[:, k : k + 1], (rows, LANES)) for k in range(begin, begin + size)
        ]
        for at in range(size):
            k = begin + at
            column = columns[at]
            inverse = 1.0 / column[k : k + 1]
            pivot_s = system[k : k + 1] * inverse
            pivot_t = target[k : k + 1] * inverse
            column = jnp.where(row == k, column - 1.0, column)
            for later in range(at + 1, size):
                columns[later] = columns[later] - column * (columns[later][k : k + 1] * inverse)
            system = system - column * pivot_s
            target = target - column * pivot_t
    return system, target


def solve_rows(system, target):
    rows = system.shape[0]
    row = lax.broadcasted_iota(jnp.int32, (rows, 1), 0)
    lane = lax.broadcasted_iota(jnp.int32, (1, rows), 1)

    def step(k, state):
        system, target = state
        column = jnp.sum(jnp.where(lane == k, system, 0.0), axis=1, keepdims=True)
        here = row == k
        inverse = 1.0 / jnp.sum(jnp.where(here, column, 0.0), axis=0, keepdims=True)
        pivot_s = jnp.sum(jnp.where(here, system, 0.0), axis=0, keepdims=True) * inverse
        pivot_t = jnp.sum(jnp.where(here, target, 0.0), axis=0, keepdims=True) * inverse
        column = jnp.where(here, column - 1.0, column)
        return system - column * pivot_s, target - column * pivot_t

    return lax.fori_loop(0, rows, step, (system, target))[1]


def others():
    heads, groups = lax.axis_size("head"), lax.axis_size("seq")
    my_head, me = lax.axis_index("head"), lax.axis_index("seq")
    for shift in range(heads):
        for step in range(groups):
            if shift or step:
                yield (
                    shift * groups + step,
                    lax.rem(my_head + shift, heads),
                    lax.rem(me + step, groups),
                )


def greet():
    barrier = pltpu.get_barrier_semaphore()
    for _, head, seq in others():
        pl.semaphore_signal(
            barrier, inc=1, device_id={"head": head, "seq": seq}, device_id_type=MESH
        )


def admit():
    pl.semaphore_wait(
        pltpu.get_barrier_semaphore(), lax.axis_size("head") * lax.axis_size("seq") - 1
    )


def send(source, target, send_sem, recv_sem, peer, head=None):
    return pltpu.make_async_remote_copy(
        src_ref=source,
        dst_ref=target,
        send_sem=send_sem,
        recv_sem=recv_sem,
        device_id={"seq": peer} if head is None else {"head": head, "seq": peer},
        device_id_type=MESH,
    )


def fit_kernel(
    sizes_hbm, owners_hbm, q_hbm, k_hbm, v_hbm, idx_hbm, p_ref, x_ref,
    sizes_ref, owners_ref, q_in, idx_ref,
    piece, table, k_ref, v_ref, s_ref, g_ref, high_ref, low_ref, t_ref,
    part, part_in, chunk_mine, chunks, gram_out, gram_in,
    e_out, e_in, pair, both, z_out, z_in, p_all, x_mine, x_all,
    load, send_q, recv_q, send_part, recv_part, send_chunk, recv_chunk, send_gram, recv_gram,
    send_e, recv_e, send_z, recv_z, send_p, recv_p, send_x, recv_x,
):
    layers, local_len, width = k_ref.shape
    fits, capacity = idx_ref.shape
    heads, my_head = lax.axis_size("head"), lax.axis_index("head")
    groups, me = lax.axis_size("seq"), lax.axis_index("seq")
    rows = groups * heads
    outer, inner = me // PAIR, lax.rem(me, PAIR)
    outers, half = groups // PAIR, fits // PAIR
    partner = outer * PAIR + 1 - inner
    fit_mine = jnp.minimum(me, fits - 1)
    chunk = layers * rows // groups
    start = me * local_len
    lane = lax.broadcasted_iota(jnp.int32, (rows, LANES), 1)
    near = (outer >= outers // 2).astype(jnp.int32)
    far = 1 - near
    inside_line = (outer > 0) & (outer < outers - 1)
    wide = gram_in.shape[2]
    middle = (rows + wide) // 2

    loads = [
        pltpu.make_async_copy(k_hbm, k_ref, load.at[0]),
        pltpu.make_async_copy(v_hbm, v_ref, load.at[1]),
        pltpu.make_async_copy(idx_hbm, idx_ref, load.at[2]),
        pltpu.make_async_copy(q_hbm, q_in, load.at[3]),
        pltpu.make_async_copy(sizes_hbm, sizes_ref, load.at[4]),
        pltpu.make_async_copy(owners_hbm, owners_ref, load.at[5]),
    ]
    loads[3].start()
    greet()
    for at in (4, 5, 2, 0, 1):
        loads[at].start()
    loads[3].wait()
    drawn_rows = q_in[...].astype(jnp.float32)
    for head in range(heads):
        for layer in range(layers):
            at = layer * heads + head
            piece[head, layer : layer + 1, :] = drawn_rows[at : at + 1]
    admit()
    my_row = me * heads + my_head
    asked = []
    for at, head, seq in others():
        asked.append(
            send(piece.at[head], table.at[my_row], send_q, recv_q, seq, head)
        )
        asked[-1].start()
    table[my_row] = piece[my_head]
    every = table.at[pl.ds(0, heads * groups - 1)]
    send(every, every, send_q, recv_q, partner).wait_recv()
    for at in (0, 2, 4, 5):
        loads[at].wait()
    for layer in range(layers):
        query_rows = table[:, layer, :].astype(jnp.bfloat16)
        s_ref[layer] = lax.dot_general(
            query_rows, k_ref[layer], NT, preferred_element_type=jnp.float32
        ) * (width ** (-0.5) * LOG2E)

    parts = [
        send(
            part.at[lax.rem(me + step, groups)], part_in.at[step],
            send_part, recv_part, lax.rem(me + step, groups),
        )
        for step in range(1, groups)
    ]

    def attend():
        loads[1].wait()
        for layer in range(layers):
            scores = s_ref[layer]
            peak = jnp.max(scores, axis=1, keepdims=True)
            weights = jnp.exp2(scores - peak)
            total = jnp.sum(weights, axis=1, keepdims=True)
            numer = jnp.dot(
                weights.astype(jnp.bfloat16), v_ref[layer], preferred_element_type=jnp.float32
            )
            side = jnp.where(lane < 64, total, peak)
            for at in range(rows // chunk):
                slot = layer * (rows // chunk) + at
                part[slot, 0] = numer[at * chunk : (at + 1) * chunk]
                part[slot, 1] = side[at * chunk : (at + 1) * chunk]
        for copy in parts:
            copy.start()
        part_in[0] = part[me]

    def produce(fit):
        layer = fit // FITS_LAYER
        size = sizes_ref[0, fit]
        offset = idx_ref[pl.ds(fit, 1), :] - start
        position = lax.broadcasted_iota(jnp.int32, (1, capacity), 1)
        inside = (offset >= 0) & (offset < local_len) & (position < size)
        high_ref[...] = jnp.broadcast_to(
            jnp.where(inside, offset >> 7, -1), (SUBLANES, capacity)
        )
        low_ref[...] = jnp.broadcast_to(offset & (LANES - 1), (SUBLANES, capacity))
        band = min(rows, BAND)

        def one_band(base_row):
            def one_tile(tile, top):
                base = pl.multiple_of(tile * LANES, LANES)
                high = high_ref[:, pl.ds(base, LANES)]
                low = low_ref[:, pl.ds(base, LANES)]
                picked = [jnp.full((SUBLANES, LANES), FAR, jnp.float32)] * (band // SUBLANES)
                for block in range(local_len // LANES):
                    here = high == block
                    for group in range(band // SUBLANES):
                        scored = s_ref[
                            layer,
                            pl.ds(base_row + group * SUBLANES, SUBLANES),
                            block * LANES : (block + 1) * LANES,
                        ]
                        found = jnp.take_along_axis(
                            scored, low, axis=1, mode="promise_in_bounds"
                        )
                        picked[group] = jnp.where(here, found, picked[group])
                joined = jnp.concatenate(picked, axis=0)
                g_ref[pl.ds(base_row, band), pl.ds(base, LANES)] = joined
                return jnp.maximum(top, joined)

            top = lax.fori_loop(
                0,
                capacity // LANES,
                one_tile,
                jnp.full((band, LANES), FAR, jnp.float32),
                unroll=True if rows == band else 1,
            )
            t_ref[pl.ds(base_row, band), :] = top

        if rows == band:
            one_band(0)
        else:

            def step(at, carry):
                one_band(pl.multiple_of(at * band, band))
                return carry

            lax.fori_loop(0, rows // band, step, 0)
        top = COARSE * jnp.ceil(jnp.max(t_ref[...], axis=1, keepdims=True) * (1.0 / COARSE))
        picked = g_ref[...]
        return jnp.where(picked > 0.5 * FAR, jnp.exp2(picked - top), 0.0), top

    gram_lane = lax.broadcasted_iota(jnp.int32, (rows, wide), 1)

    def gram_copy(j):
        return send(gram_out.at[j], gram_in.at[outer], send_gram, recv_gram, keeps[j])

    def fill_gram(j):
        expo = both[j, :, :capacity]
        top = both[j, :, capacity:].astype(jnp.float32)[:, :1]
        total = jnp.sum(expo.astype(jnp.float32), axis=1, keepdims=True)
        gram_out[j] = jnp.where(gram_lane >= middle, top, total)
        gram_out[j, :, :rows] = lax.dot_general(
            expo, expo, NT, preferred_element_type=jnp.float32
        )
        pl.when(keeps[j] != me)(gram_copy(j).start)

    cut = capacity // 2
    spans = (slice(cut, capacity + LANES), slice(0, cut))
    plain = (slice(cut, capacity), slice(0, cut))
    gives = [j * PAIR + 1 - inner for j in range(half)]
    keeps = [j * PAIR + inner for j in range(half)]

    def cross(j, q):
        return send(
            e_out.at[j, :, spans[q]], e_in.at[j, :, spans[q]],
            send_e, recv_e.at[j, q], partner,
        )

    def stream(way, j, q):
        return send(
            z_out.at[way, j, :, spans[q]], z_in.at[way, j, :, spans[q]],
            send_z.at[way], recv_z.at[way, j, q],
            lax.rem(me + PAIR * (1 - 2 * way) + groups, groups),
        )

    def onward(j, q):
        return send(
            p_all.at[keeps[j], :, plain[q]], p_all.at[keeps[j], :, plain[q]],
            send_p, recv_p, partner,
        )

    def sent(ref, sem):
        send(ref, ref, sem, sem, partner).wait_send()

    def came(ref, sem):
        send(ref, ref, sem, sem, partner).wait_recv()

    def scales(one, other):
        first = one[:, capacity:].astype(jnp.float32)
        second = other[:, capacity:].astype(jnp.float32)
        top = jnp.maximum(first, second)
        wide_by = cut // LANES
        return (
            top.astype(jnp.bfloat16),
            jnp.concatenate([jnp.exp2(first - top).astype(jnp.bfloat16)] * wide_by, axis=1),
            jnp.concatenate([jnp.exp2(second - top).astype(jnp.bfloat16)] * wide_by, axis=1),
        )

    def blend(one, other, at):
        top, first, second = scales(one, other)
        return one[:, at] * first + other[:, at] * second, top

    def put(ref, q, mixed):
        ref[:, plain[q]] = mixed[0]
        if q == 0:
            ref[:, capacity:] = mixed[1]

    def tail_of(top):
        return jnp.broadcast_to(top, (rows, LANES)).astype(jnp.bfloat16)

    def give(j):
        expo, top = produce(gives[j])
        expo = expo.astype(jnp.bfloat16)
        e_out[j, :, :capacity] = expo
        e_out[j, :, capacity:] = tail_of(top)
        for q in range(2):
            cross(j, q).start()

    def keep(j):
        expo, top = produce(keeps[j])
        expo = expo.astype(jnp.bfloat16)
        pair[j, :, :capacity] = expo
        pair[j, :, capacity:] = tail_of(top)

    def join(j, q):
        cross(j, q).wait_recv()
        mixed = blend(pair.at[j], e_in.at[j], plain[q])
        put(both.at[j], q, mixed)

        @pl.when(~inside_line)
        def _():
            put(z_out.at[near, j], q, mixed)
            stream(near, j, q).start()

        if q == 1:
            fill_gram(j)

    def pass_near(j, q):

        @pl.when(inside_line)
        def _():
            stream(near, j, q).wait_recv()
            put(z_out.at[near, j], q, blend(both.at[j], z_in.at[near, j], plain[q]))
            stream(near, j, q).start()

    def pass_far(j, q):
        stream(far, j, q).wait_recv()

        @pl.when(inside_line)
        def _():
            put(z_out.at[far, j], q, blend(both.at[j], z_in.at[far, j], plain[q]))
            stream(far, j, q).start()

        p_all[keeps[j], :, plain[q]] = blend(z_out.at[near, j], z_in.at[far, j], plain[q])[0]
        onward(j, q).start()

    def merge_targets():
        came(part_in.at[pl.ds(1, groups - 1)], recv_part)
        peak = part_in[0, 1][:, 64:65]
        for step in range(1, groups):
            peak = jnp.maximum(peak, part_in[step, 1][:, 64:65])
        numer, total = 0.0, 0.0
        for step in range(groups):
            factor = jnp.exp2(part_in[step, 1][:, 64:65] - peak)
            numer = numer + part_in[step, 0] * factor
            total = total + part_in[step, 1][:, 0:1] * factor
        target = numer / total
        chunk_mine[...] = target
        chunks[me] = target
        for copy in spread:
            copy.start()

    spread = [
        send(
            chunk_mine, chunks.at[me], send_chunk, recv_chunk,
            lax.rem(me + step, groups),
        )
        for step in range(1, groups)
    ]
    results = [
        send(
            x_mine, x_all.at[fit_mine], send_x, recv_x,
            lax.rem(me + step, groups),
        )
        for step in range(1, groups)
    ]

    def only(condition, act):
        if groups == fits:
            act()
        else:
            pl.when(condition)(act)

    def gather_system():
        came(chunks.at[pl.ds(0, groups - 1)], recv_chunk)

        def wait_grams():
            came(gram_in.at[pl.ds(0, outers - 1)], recv_gram)

        only(me < fits, wait_grams)

    state = {}

    def assemble():
        diagonal = lax.broadcasted_iota(jnp.int32, (rows, wide), 0) == lax.broadcasted_iota(
            jnp.int32, (rows, wide), 1
        )

        def across_lanes(column):
            return jnp.sum(jnp.where(diagonal, column, 0.0), axis=0, keepdims=True)

        gram_in[outer] = gram_out[jnp.minimum(outer, half - 1)]
        tops = [gram_in[source, :, middle : middle + 1] for source in range(outers)]
        top = tops[0]
        for other in tops[1:]:
            top = jnp.maximum(top, other)
        gram, total = 0.0, 0.0
        for source in range(outers):
            factor = jnp.exp2(tops[source] - top)
            total = total + factor * gram_in[source, :, rows : rows + 1]
            gram = gram + gram_in[source] * factor * across_lanes(factor)
        scale = 1.0 / total
        gram = jnp.where(gram_lane < rows, gram * scale * across_lanes(scale), 0.0)
        trace = jnp.sum(jnp.where(diagonal, gram, 0.0))
        ridge = RIDGE * trace / sizes_ref[0, fit_mine].astype(jnp.float32)
        span = rows // chunk
        base = (fit_mine // FITS_LAYER) * span
        target = jnp.concatenate([chunks[base + at] for at in range(span)], axis=0)
        state["target"] = target.astype(jnp.bfloat16).astype(jnp.float32)
        state["system"] = jnp.where(diagonal, gram + ridge, gram)
        state["scale"] = scale

    def conclude(solved):
        solved = solved * state["scale"]
        x_mine[...] = solved
        x_all[fit_mine] = solved
        for copy in results:
            copy.start()

    small = rows <= 64 and groups == fits

    def solve_first():
        gather_system()
        if small:
            assemble()
            state["system"], state["target"] = eliminate(
                state["system"], state["target"], 0, rows // 2
            )

    def solve_last():
        if small:
            conclude(eliminate(state["system"], state["target"], rows // 2, rows)[1])
        else:

            def whole():
                assemble()
                conclude(solve_rows(state["system"][:, :rows], state["target"]))

            only(me < fits, whole)

    agenda = [(1.37, attend, ()), (7.21, merge_targets, ())]
    agenda += [(15.23, solve_first, ()), (16.17, solve_last, ())]
    for j in range(half):
        agenda += [(1.39 * j, give, (j,)), (3.86 + 1.87 * j, keep, (j,))]
        for q in range(2):
            at = 3.92 + 1.95 * j + 0.65 * q
            agenda.append((at, join, (j, q)))
            agenda.append((at + 3.56, pass_near, (j, q)))
            agenda.append((at + 6.84, pass_far, (j, q)))
    for _, act, at in sorted(agenda, key=lambda entry: entry[0]):
        act(*at)
    sent(table.at[pl.ds(0, heads * groups - 1)], send_q)
    sent(part.at[pl.ds(0, groups - 1)], send_part)
    sent(chunks.at[pl.ds(0, groups - 1)], send_chunk)
    sent(e_out, send_e)
    if groups == fits:
        sent(gram_out.at[pl.ds(0, half - 1)], send_gram)
    else:
        pl.when(me < fits)(lambda: sent(gram_out.at[pl.ds(0, half - 1)], send_gram))
        pl.when(me >= fits)(lambda: sent(gram_out, send_gram))
    sent(z_out.at[near], send_z.at[near])
    pl.when(inside_line)(lambda: sent(z_out.at[far], send_z.at[far]))
    sent(p_all.at[pl.ds(0, half)], send_p)
    if groups == fits:
        came(x_all.at[pl.ds(0, fits - 1)], recv_x)
        sent(x_all.at[pl.ds(0, groups - 1)], send_x)
    else:
        pl.when(me < fits)(lambda: came(x_all.at[pl.ds(0, fits - 1)], recv_x))
        pl.when(me < fits)(lambda: [copy.wait_send() for copy in results] and None)
        pl.when(me >= fits)(lambda: came(x_all, recv_x))
    came(p_all.at[pl.ds(0, half)], recv_p)
    count = jnp.int32(0)
    chosen = [jnp.int32(0)] * SLOTS
    for fit in range(fits):
        mine = owners_ref[0, fit] == me
        for slot in range(SLOTS):
            chosen[slot] = jnp.where(mine & (count == slot), fit, chosen[slot])
        count = count + mine.astype(jnp.int32)
    for slot in range(SLOTS):
        p_ref[slot] = p_all[chosen[slot]]
        x_ref[slot] = jnp.where(count > slot, x_all[chosen[slot]], 0.0)


def place_kernel(p_ref, x_ref, out_hbm, out_ref, store):
    stores = []
    for slot in range(SLOTS):
        probs = p_ref[slot]
        rows = x_ref[slot]
        high = rows.astype(jnp.bfloat16)
        low = (rows - high.astype(jnp.float32)).astype(jnp.bfloat16)
        out_ref[slot] = lax.dot_general(
            jnp.concatenate([probs, probs], axis=0),
            jnp.concatenate([high, low], axis=0),
            TN,
            preferred_element_type=jnp.float32,
        ).astype(jnp.bfloat16)
        stores.append(pltpu.make_async_copy(out_ref.at[slot], out_hbm.at[0, slot], store.at[slot]))
        stores[-1].start()
    for copy in stores:
        copy.wait()


VMEM = pl.BlockSpec(memory_space=pltpu.VMEM)
ANY = pl.BlockSpec(memory_space=pl.ANY)


def on_device(queries, keys, values, indices, sizes, owners):
    layers, heads, count, width = queries.shape
    groups = lax.axis_size("seq")
    rows = groups * heads * count
    local_len = keys.shape[2]
    fits, capacity = indices.shape[1:]
    dma = pltpu.SemaphoreType.DMA
    params = dict(vmem_limit_bytes=(24 + rows // 8) * 1024 * 1024)
    outers, half = groups // PAIR, fits // PAIR
    chunk = layers * rows // groups
    wide = (rows // LANES + 1) * LANES
    packed = (rows, capacity + LANES)
    probs, solved = pl.pallas_call(
        fit_kernel,
        out_shape=(
            jax.ShapeDtypeStruct((SLOTS, rows, capacity), jnp.bfloat16),
            jax.ShapeDtypeStruct((SLOTS, rows, width), jnp.float32),
        ),
        in_specs=[ANY] * 6,
        out_specs=(VMEM, VMEM),
        scratch_shapes=[
            pltpu.SMEM((1, fits), jnp.int32),
            pltpu.SMEM((1, fits), jnp.int32),
            pltpu.VMEM((layers * heads, width), queries.dtype),
            pltpu.VMEM((fits, capacity), jnp.int32),
            pltpu.VMEM((heads, layers, width), jnp.float32),
            pltpu.VMEM((rows, layers, width), jnp.float32),
            pltpu.VMEM((layers, local_len, width), jnp.bfloat16),
            pltpu.VMEM((layers, local_len, width), jnp.bfloat16),
            pltpu.VMEM((layers, rows, local_len), jnp.float32),
            pltpu.VMEM((rows, capacity), jnp.float32),
            pltpu.VMEM((SUBLANES, capacity), jnp.int32),
            pltpu.VMEM((SUBLANES, capacity), jnp.int32),
            pltpu.VMEM((rows, LANES), jnp.float32),
            pltpu.VMEM((groups, 2, chunk, width), jnp.float32),
            pltpu.VMEM((groups, 2, chunk, width), jnp.float32),
            pltpu.VMEM((chunk, width), jnp.float32),
            pltpu.VMEM((groups, chunk, width), jnp.float32),
            pltpu.VMEM((half, rows, wide), jnp.float32),
            pltpu.VMEM((outers, rows, wide), jnp.float32),
            pltpu.VMEM((half,) + packed, jnp.bfloat16),
            pltpu.VMEM((half,) + packed, jnp.bfloat16),
            pltpu.VMEM((half,) + packed, jnp.bfloat16),
            pltpu.VMEM((half,) + packed, jnp.bfloat16),
            pltpu.VMEM((2, half) + packed, jnp.bfloat16),
            pltpu.VMEM((2, half) + packed, jnp.bfloat16),
            pltpu.VMEM((fits, rows, capacity), jnp.bfloat16),
            pltpu.VMEM((rows, width), jnp.float32),
            pltpu.VMEM((fits, rows, width), jnp.float32),
            dma((6,)),
            dma,
            dma,
            dma,
            dma,
            dma,
            dma,
            dma,
            dma,
            dma,
            dma((half, 2)),
            dma((2,)),
            dma((2, half, 2)),
            dma,
            dma,
            dma,
            dma,
        ],
        compiler_params=pltpu.CompilerParams(collective_id=2, has_side_effects=True, **params),
    )(
        *(
            pltpu.with_memory_space_constraint(array, pltpu.HBM)
            for array in (
                sizes,
                owners,
                queries.reshape(layers * heads, width),
                keys[:, 0],
                values[:, 0],
                indices[0],
            )
        )
    )
    return pl.pallas_call(
        place_kernel,
        out_shape=jax.ShapeDtypeStruct((1, SLOTS, capacity, width), jnp.bfloat16),
        in_specs=[VMEM, VMEM],
        out_specs=ANY,
        scratch_shapes=[pltpu.VMEM((SLOTS, capacity, width), jnp.bfloat16), dma((SLOTS,))],
        compiler_params=pltpu.CompilerParams(**params),
    )(probs, solved)


def solution(mesh):
    in_specs = (
        P(None, None, ("head", "seq"), None),
        P(None, "head", "seq", None),
        P(None, "head", "seq", None),
        P("head", None, None),
        P("head", None),
        P("head", None),
    )
    out_specs = P("head", "seq", None, None)
    return jax.shard_map(
        on_device, mesh=mesh, in_specs=in_specs, out_specs=out_specs, check_vma=False
    )
```
